32 devices in a mesh: ep: 4 (over y, core), fs: 8 (over z, x).
Axes of the slice: x: 2, y: 2, z: 4, core: 2. Of those that a mesh axis runs over, the one named last changes fastest.
Arguments:
- grads: bfloat16 [4, 4, 128, 14336], P('ep', None, 'fs'), may hold values from -64 to 64
- counts: int32 [4, 4], replicated, may hold values from 16 to 2047
- weight: bfloat16 [4, 128, 14336], P('ep', 'fs'), may hold values from -3 to 3
- mom: float32 [4, 128, 14336], P('ep', 'fs'), may hold values from -64 to 64
- second: float32 [4, 128, 14336], P('ep', 'fs'), may hold values from 0.1 to 10
- in_weight: float32 [6, 32], replicated, may hold values from -2.5 to 2.5
- in_bias: float32 [32], replicated, may hold values from -3 to 3
- out_weight: float32 [32, 2], replicated, may hold values from -1 to 1
- out_bias: float32 [2], replicated, may hold values from -3 to 3
Outputs:
- new_weight: bfloat16 [4, 128, 14336], P('ep')
- new_mom: float32 [4, 128, 14336], P('ep', 'fs')
- new_second: float32 [4, 128, 14336], P('ep', 'fs')
The draws below stay inside these ranges and needn't reach their ends.
All inputs are finite; a program needn't handle non-finite values.
Results may differ from the reference program's by a relative error of at most 0.0019.
Values may be sent and summed in bfloat16 or wider, within the bound.
A program may use at most 64 MiB of HBM per device.

```python
import math
import jax
import jax.numpy as jnp
from jax import lax

FF = 14336
EXPERTS = 4
R = 128
HID = 32
FEATS = 6


def scaled_field(key, field_shape, magnitude):
    key_noise, key_cols = jax.random.split(key, 2)
    row_scale = 10.0 ** (jnp.arange(R, dtype=jnp.float32) / R)
    col_scale = jnp.exp(jax.random.uniform(key_cols, (FF,), jnp.float32, 0.0, math.log(10.0)))
    noise_field = jnp.clip(jax.random.normal(key_noise, field_shape, jnp.float32), -6.0, 6.0)
    return magnitude * noise_field * row_scale[:, None] * col_scale


def draw_grads(key, part):
    return scaled_field(jax.random.fold_in(key, 101), (EXPERTS, EXPERTS, R, FF), 0.01).astype(jnp.bfloat16)


def draw_mom(key, part):
    return scaled_field(jax.random.fold_in(key, 202), (EXPERTS, R, FF), 0.01)


def touch_ends(array, stream_key, least, top_value):
    index_at = [jax.random.randint(jax.random.fold_in(stream_key, axis), (), 0, length) for axis, length in enumerate(array.shape)]
    longest = array.shape.index(max(array.shape))
    neighbour = index_at[:longest] + [(index_at[longest] + 1) % array.shape[longest]] + index_at[longest + 1:]
    return array.at[tuple(index_at)].set(least).at[tuple(neighbour)].set(top_value)


def level_of(rng, shape, cuts, smallest, top_value):
    factor_of = 1.0
    for position, shards_of in cuts:
        draws = jax.random.uniform(jax.random.fold_in(jax.random.fold_in(rng, 6), position), (shards_of,), jnp.float32, smallest / len(cuts), top_value / len(cuts))
        factor_of = factor_of * jnp.repeat(jnp.exp(draws), shape[position] // shards_of).reshape((-1,) + (1,) * (len(shape) - 1 - position))
    return factor_of


def noise(stream_key, shape, spread, most, cuts=(), held_as=jnp.bfloat16):
    values = jax.random.normal(stream_key, shape, jnp.float32) * spread
    if len(cuts) > 0:
        values = level_of(stream_key, shape, cuts, -0.22, 0.18) * values
    return jnp.clip(values, min=-most, max=most).astype(held_as)


def setup_inputs(seed: int = 0) -> dict:
    key_list = jax.random.split(jax.random.key(seed), 10)
    return {
        "grads": draw_grads(jax.random.fold_in(key_list[9], 71), 0),
        "counts": touch_ends(jax.random.randint(key_list[1], (EXPERTS, EXPERTS), 16, 2048), jax.random.fold_in(key_list[1], 1), 16, 2047).astype(jnp.int32),
        "weight": noise(key_list[2], (EXPERTS, R, FF), 0.5, 3.0, ((0, 4), (1, 8))),
        "mom": draw_mom(jax.random.fold_in(key_list[9], 71), 0),
        "second": jnp.clip(jnp.exp(math.log(10.0) - 4.6051702 * jax.random.uniform(key_list[4], (EXPERTS, R, FF), jnp.float32) ** level_of(key_list[4], (EXPERTS, R, FF), ((0, 4), (1, 8)), -0.2, 0.2)), 0.1, 10.0),
        "in_weight": noise(key_list[5], (FEATS, HID), FEATS ** -0.5, 2.5, (), jnp.float32),
        "in_bias": noise(key_list[6], (HID,), 0.5, 3.0, (), jnp.float32),
        "out_weight": noise(key_list[7], (HID, 2), HID ** -0.5, 1.0, (), jnp.float32),
        "out_bias": noise(key_list[8], (2,), 0.5, 3.0, (), jnp.float32),
    }


MOMENTUM_DECAY = 0.9
SECOND_DECAY = 0.99
NORM_EPS = 1e-06
ROOT_EPS = 1e-08
STEP_SCALE = 0.2
EXP_SCALE = 0.5

def learned_step(gradient, mom_next, second_next, weight, grad_norm, mom_norm, in_weight, in_bias, out_weight, out_bias):
    inv_root = lax.rsqrt(second_next + ROOT_EPS)
    features = jnp.stack([gradient / grad_norm, mom_next / mom_norm, mom_next * inv_root, gradient * inv_root, weight.astype(jnp.float32), jnp.broadcast_to(jnp.log(mom_norm), gradient.shape)])
    hidden = jax.nn.relu(jnp.einsum('fh,fab->hab', in_weight, features, precision=lax.Precision.HIGHEST) + in_bias[:, None, None])
    outputs = jnp.einsum('hk,hab->kab', out_weight, hidden, precision=lax.Precision.HIGHEST) + out_bias[:, None, None]
    update = STEP_SCALE * outputs[0] * jnp.exp(EXP_SCALE * outputs[1])
    return (weight.astype(jnp.float32) - update).astype(jnp.bfloat16)

def reference(grads, counts, weight, mom, second, in_weight, in_bias, out_weight, out_bias):
    counts_f = counts.astype(jnp.float32)
    totals = lax.optimization_barrier(jnp.sum(counts_f, axis=0))
    shares = counts_f / totals[None, :]

    def per_expert(items):
        expert_grads, expert_shares, expert_weight, expert_mom, expert_second = items
        weighted = (expert_shares[:, None, None] * expert_grads.astype(jnp.float32)).astype(jnp.bfloat16)
        weighted = lax.optimization_barrier(weighted)
        gradient = lax.optimization_barrier(jnp.sum(weighted.astype(jnp.float32), axis=0))
        mom_next = MOMENTUM_DECAY * expert_mom + (1.0 - MOMENTUM_DECAY) * gradient
        second_next = SECOND_DECAY * expert_second + (1.0 - SECOND_DECAY) * gradient * gradient
        entries = gradient.shape[0] * gradient.shape[1]
        grad_norm = jnp.sqrt(jnp.sum(gradient * gradient) / entries + NORM_EPS)
        mom_norm = jnp.sqrt(jnp.sum(mom_next * mom_next) / entries + NORM_EPS)
        updated = learned_step(gradient, mom_next, second_next, expert_weight, grad_norm, mom_norm, in_weight, in_bias, out_weight, out_bias)
        return (updated, mom_next, second_next)
    new_weight, new_mom, new_second = lax.map(per_expert, (jnp.swapaxes(grads, 0, 1), shares.T, weight, mom, second))
    return (new_weight, new_mom, new_second)
```

```python
import functools

import jax
import jax.numpy as jnp
from jax import lax
from jax.experimental import pallas as pl
from jax.experimental.pallas import tpu as pltpu
from jax.sharding import PartitionSpec as P

MOMENTUM_DECAY = 0.9
SECOND_DECAY = 0.99
NORM_EPS = 1e-06
ROOT_EPS = 1e-08
STEP_SCALE = 0.2
EXP_SCALE = 0.5
LANES = 128
CORES = 2
MOST_CHUNKS = 28
MOST_CUTS = 14
LAG = 4
TURN_LAG = 4
VMEM_BYTES = 67043328
FLUSH_BYTES = 1 << 20


def largest_divisor(number, most):
    return max(d for d in range(1, most + 1) if number % d == 0)


def tile_width(columns, most):
    return LANES * largest_divisor(columns // LANES, most // LANES)


def turned_chunks(depth, across, chunks):
    def load(turned):
        straight = chunks - turned
        on_x = (across - 1) * (depth * straight + turned)
        on_z = (depth - 1) * (straight + across * turned)
        return max(on_x, on_z)

    return min(range(chunks + 1), key=load)


def remote(src, dst, send_sem, recv_sem, axis, peer):
    return pltpu.make_async_remote_copy(
        src_ref=src,
        dst_ref=dst,
        send_sem=send_sem,
        recv_sem=recv_sem,
        device_id={axis: peer},
        device_id_type=pl.DeviceIdType.MESH,
    )


def signal(semaphore, axis, peer):
    pl.semaphore_signal(
        semaphore, inc=1, device_id={axis: peer}, device_id_type=pl.DeviceIdType.MESH
    )


def kernel(
    groups,
    depth,
    across,
    chunks,
    counts_hbm,
    in_weight_hbm,
    in_bias_hbm,
    out_weight_hbm,
    out_bias_hbm,
    grads_hbm,
    weight_hbm,
    mom_hbm,
    second_hbm,
    gathered,
    mom,
    second,
    counts,
    in_weight,
    in_bias,
    out_weight,
    out_bias,
    grads,
    weight,
    handed,
    taken,
    outgoing,
    arrived,
    gradient,
    sums,
    bias,
    small_sem,
    slab_sem,
    param_sem,
    pair_send,
    pair_recv,
    grad_send,
    grad_recv,
    chain,
    sum_send,
    sum_recv,
    row_send,
    row_recv,
):
    shards = depth * across
    planes = groups // CORES
    rows, columns = mom.shape
    units = in_bias.shape[0]
    me_group = lax.axis_index("ep")
    plane = me_group // CORES
    core = me_group % CORES
    partner = plane * CORES + (CORES - 1 - core)
    me = lax.axis_index("fs")
    z = me // across
    x = me % across

    def own_of(step):
        return (plane + step) % planes * CORES + core

    def other_of(step):
        return (plane + step) % planes * CORES + (CORES - 1 - core)

    barrier = pltpu.get_barrier_semaphore()
    signal(barrier, "ep", partner)
    for step in range(1, planes):
        signal(barrier, "ep", own_of(step))
    for step in range(1, across):
        signal(barrier, "fs", z * across + (x + step) % across)

    @pl.when(z < depth - 1)
    def _():
        signal(barrier, "fs", me + across)

    @pl.when(z > 0)
    def _():
        signal(barrier, "fs", me - across)

    small = [
        pltpu.make_async_copy(src, dst, small_sem.at[i])
        for i, (src, dst) in enumerate(
            (
                (counts_hbm, counts),
                (in_weight_hbm, in_weight),
                (in_bias_hbm, in_bias),
                (out_weight_hbm, out_weight),
                (out_bias_hbm, out_bias),
            )
        )
    ]
    for copy in small:
        copy.start()

    order = [*range(1, planes), 0]
    slabs = [
        pltpu.make_async_copy(
            grads_hbm.at[0, expert_of(step)], grads.at[kind, step], slab_sem.at[kind, step]
        )
        for kind, expert_of in enumerate((other_of, own_of))
        for step in order
    ]
    for copy in slabs:
        copy.start()
    params = [
        pltpu.make_async_copy(src.at[0], dst, param_sem.at[i])
        for i, (src, dst) in enumerate(
            (
                (mom_hbm, mom),
                (second_hbm, second),
                (weight_hbm, weight),
            )
        )
    ]
    for copy in params:
        copy.start()

    cuts = grad_recv.shape[1]
    cut = columns // cuts
    narrow = tile_width(cut, 512)

    def cols_of(c, i):
        return pl.ds(pl.multiple_of(c * cut + i * narrow, narrow), narrow)

    def piece_of(c):
        return pl.ds(pl.multiple_of(c * cut, cut), cut)

    for copy in small:
        copy.wait()

    def share_of(expert):
        total = counts[0, expert]
        for s in range(1, groups):
            total = total + counts[s, expert]
        mine = jnp.full((1, LANES), counts[me_group, expert].astype(jnp.float32))
        return (mine / jnp.full((1, LANES), total.astype(jnp.float32)))[:, :1]

    shares = [
        [share_of(expert_of(step)) for step in range(planes)] for expert_of in (other_of, own_of)
    ]

    def weighted(kind, step, cols):
        value = shares[kind][step] * grads[kind, step, :, cols].astype(jnp.float32)
        return value.astype(jnp.bfloat16)

    for copy in slabs[:planes]:
        copy.wait()

    def hand(i, carry):
        cols = pl.ds(pl.multiple_of(i * narrow, narrow), narrow)
        for step in order:
            handed[step, :, cols] = weighted(0, step, cols)
        return carry

    lax.fori_loop(0, columns // narrow, hand, 0)
    for copy in slabs[planes:]:
        copy.wait()

    near = 1 + (planes - 1) + (across - 1)
    near = near + (z > 0).astype(jnp.int32) + (z < depth - 1).astype(jnp.int32)
    pl.semaphore_wait(barrier, near)

    def pair_copy(step, c):
        return remote(
            handed.at[step, :, piece_of(c)],
            taken.at[step, :, piece_of(c)],
            pair_send.at[step, c],
            pair_recv.at[step, c],
            "ep",
            partner,
        )

    def grad_copy(step, c):
        return remote(
            outgoing.at[step - 1, :, piece_of(c)],
            arrived.at[step - 1, :, piece_of(c)],
            grad_send.at[step - 1, c],
            grad_recv.at[step - 1, c],
            "ep",
            own_of(step),
        )

    def start_pairs(c, carry):
        for step in order[:-1]:
            pair_copy(step, c).start()
        return carry

    lax.fori_loop(0, cuts, start_pairs, 0)

    def start_own(c, carry):
        pair_copy(0, c).start()
        return carry

    lax.fori_loop(0, cuts, start_own, 0)

    def send_piece(c, carry):
        for step in order[:-1]:
            pair_copy(step, c).wait_recv()

            def add(i, inner, step=step):
                cols = cols_of(c, i)
                total = weighted(1, step, cols).astype(jnp.float32)
                total = total + taken[step, :, cols].astype(jnp.float32)
                outgoing[step - 1, :, cols] = total.astype(jnp.bfloat16)
                return inner

            lax.fori_loop(0, cut // narrow, add, 0)
            grad_copy(step, c).start()
        return carry

    lax.fori_loop(0, cuts, send_piece, 0)

    @pl.when(z > 0)
    def _():
        pl.semaphore_wait(chain.at[0], 1)

    @pl.when(z < depth - 1)
    def _():
        signal(chain.at[0], "fs", me + across)
        pl.semaphore_wait(chain.at[1], 1)

    @pl.when(z > 0)
    def _():
        signal(chain.at[1], "fs", me - across)

    def gather_own(c, carry):
        pair_copy(0, c).wait_recv()

        def one(i, inner):
            cols = cols_of(c, i)
            gradient[:, cols] = weighted(1, 0, cols).astype(jnp.float32) + taken[
                0, :, cols
            ].astype(jnp.float32)
            return inner

        return lax.fori_loop(0, cut // narrow, one, carry)

    lax.fori_loop(0, cuts, gather_own, 0)
    for copy in params:
        copy.wait()

    def moments(c, carry):
        for step in range(1, planes):
            grad_copy(step, c).wait_recv()

        def one(i, inner):
            grad_acc, mom_acc = inner
            cols = cols_of(c, i)
            total = gradient[:, cols]
            for step in range(1, planes):
                total = total + arrived[step - 1, :, cols].astype(jnp.float32)
            mom_next = MOMENTUM_DECAY * mom[:, cols] + (1.0 - MOMENTUM_DECAY) * total
            gradient[:, cols] = total
            mom[:, cols] = mom_next
            second[:, cols] = (
                SECOND_DECAY * second[:, cols] + (1.0 - SECOND_DECAY) * total * total
            )
            return grad_acc + total * total, mom_acc + mom_next * mom_next

        return lax.fori_loop(0, cut // narrow, one, carry)

    zero = jnp.zeros((rows, narrow), jnp.float32)
    grad_acc, mom_acc = lax.fori_loop(0, cuts, moments, (zero, zero))

    def to_lanes(acc):
        acc = jnp.sum(acc, axis=0, keepdims=True)
        return sum(acc[:, j : j + LANES] for j in range(0, narrow, LANES))

    sums[me, 0:1, :] = to_lanes(grad_acc)
    sums[me, 1:2, :] = to_lanes(mom_acc)
    sum_sends = []
    for step in range(1, shards):
        copy = remote(
            sums.at[me],
            sums.at[me],
            sum_send.at[step - 1],
            sum_recv.at[me],
            "fs",
            (me + step) % shards,
        )
        copy.start()
        sum_sends.append(copy)
    for step in range(1, shards):
        source = (me + step) % shards
        remote(
            sums.at[source],
            sums.at[source],
            sum_send.at[step - 1],
            sum_recv.at[source],
            "fs",
            source,
        ).wait_recv()

    entries = rows * columns * shards
    totals = sums[0]
    for s in range(1, shards):
        totals = totals + sums[s]
    mean = jnp.broadcast_to(jnp.sum(totals, axis=1, keepdims=True) / entries, (2, LANES)) + NORM_EPS
    inverse = lax.rsqrt(mean)
    inv_grad = inverse[0:1, :1]
    inv_mom = inverse[1:2, :1]
    log_mom = jnp.max(0.5 * jnp.log(mean[1:2, :]))
    for h in range(units):
        bias[h] = in_bias[h] + in_weight[5, h] * log_mom

    width = columns // chunks
    tile = tile_width(width, 256)

    def learned_step(cols):
        grad = gradient[:, cols]
        mom_next = mom[:, cols]
        old = weight[:, cols].astype(jnp.float32)
        inv_root = lax.rsqrt(second[:, cols] + ROOT_EPS)
        features = (
            grad * inv_grad,
            mom_next * inv_mom,
            mom_next * inv_root,
            grad * inv_root,
            old,
        )
        direction = jnp.full(grad.shape, out_bias[0])
        magnitude = jnp.full(grad.shape, out_bias[1])
        for h in range(units):
            hidden = features[0] * in_weight[0, h] + bias[h]
            for f in range(1, len(features)):
                hidden = hidden + features[f] * in_weight[f, h]
            hidden = jnp.maximum(hidden, 0.0)
            direction = direction + hidden * out_weight[0, h]
            magnitude = magnitude + hidden * out_weight[1, h]
        update = STEP_SCALE * direction * jnp.exp(EXP_SCALE * magnitude)
        return (old - update).astype(jnp.bfloat16)

    def rows_of(source):
        return pl.ds(pl.multiple_of(source * rows, rows), rows)

    ways = (
        (across, z < depth - 1),
        (-across, z > 0),
        (1, x < across - 1),
        (-1, x > 0),
    )
    turned = turned_chunks(depth, across, chunks)
    period = chunks // turned if turned else chunks
    along_z = (z, depth, across, (0, 1))
    along_x = (x, across, 1, (2, 3))
    trees = ((along_x, along_z, turned), (along_z, along_x, chunks - turned))

    def in_tree(tree, k):
        if not turned:
            return k >= 0 if tree else k < 0
        chosen = jnp.logical_and(k % period == period // 2, k // period < turned)
        return jnp.logical_not(chosen) if tree else chosen

    def block(source, k):
        return gathered.at[rows_of(source), pl.ds(pl.multiple_of(k * width, width), width)]

    def send(tree, source, k, which):
        for number in which:
            offset, possible = ways[number]

            @pl.when(possible)
            def _(number=number, offset=offset):
                piece = block(source, k)
                remote(
                    piece,
                    piece,
                    row_send.at[tree, number, source],
                    row_recv.at[source, k],
                    "fs",
                    me + offset,
                ).start()

    def await_block(source, k):
        piece = block(source, k)
        remote(
            piece, piece, row_send.at[0, 0, source], row_recv.at[source, k], "fs", source
        ).wait_recv()

    def live(tree, k):
        inside = jnp.logical_and(k >= 0, k < chunks)
        return jnp.logical_and(inside, in_tree(tree, jnp.maximum(k, 0)))

    def relay(t, tree):
        first, second, count = trees[tree]
        if not count:
            return
        at, size, stride, (up, down) = first
        other, length, pitch, (up_other, down_other) = second
        lag = LAG if tree else TURN_LAG
        for d in range(size - 1, 0, -1):
            k = t - lag * d

            @pl.when(live(tree, k))
            def _(d=d, k=k):
                @pl.when(at >= d)
                def _():
                    source = me - d * stride
                    await_block(source, k)
                    send(tree, source, k, (up,) + second[3])

                @pl.when(at + d < size)
                def _():
                    source = me + d * stride
                    await_block(source, k)
                    send(tree, source, k, (down,) + second[3])

        for e in range(length - 2, 0, -1):
            k = t - lag * (size - 1) - LAG * e

            @pl.when(live(tree, k))
            def _(e=e, k=k):
                for level in range(size):

                    @pl.when(jnp.logical_and(other >= e, other < length - 1))
                    def _(level=level):
                        source = level * stride + (other - e) * pitch
                        await_block(source, k)
                        send(tree, source, k, (up_other,))

                    @pl.when(jnp.logical_and(other + e < length, other > 0))
                    def _(level=level):
                        source = level * stride + (other + e) * pitch
                        await_block(source, k)
                        send(tree, source, k, (down_other,))

    def turn(t, carry):
        @pl.when(t < chunks)
        def _():
            def one(i, inner):
                cols = pl.ds(pl.multiple_of(t * width + i * tile, tile), tile)
                gathered[rows_of(me), cols] = learned_step(cols)
                return inner

            lax.fori_loop(0, width // tile, one, 0)

        for tree in range(2):

            @pl.when(live(tree, t))
            def _(tree=tree):
                send(tree, me, t, (0, 1, 2, 3))

        for tree in (1, 0):
            relay(t, tree)
        return carry

    reach = max(
        LAG * (depth - 1) + LAG * max(across - 2, 0),
        TURN_LAG * (across - 1) + LAG * max(depth - 2, 0),
    )
    lax.fori_loop(0, chunks + reach, turn, 0)

    def finish(k, carry):
        for tree in range(2):
            first, second, count = trees[tree]
            _, size, stride, _ = first
            other, length, pitch, _ = second

            @pl.when(in_tree(tree, k))
            def _(size=size, stride=stride, other=other, length=length, pitch=pitch):
                for level in range(size):
                    for place in range(length):
                        below = jnp.logical_and(place < other, other == length - 1)
                        above = jnp.logical_and(place > other, other == 0)

                        @pl.when(jnp.logical_or(below, above))
                        def _(level=level, place=place):
                            await_block(level * stride + place * pitch, k)

        return carry

    lax.fori_loop(0, chunks, finish, 0)

    def drain(c, carry):
        for step in range(planes):
            pair_copy(step, c).wait_send()
        for step in range(1, planes):
            grad_copy(step, c).wait_send()
        return carry

    lax.fori_loop(0, cuts, drain, 0)
    for copy in sum_sends:
        copy.wait_send()
    for tree in range(2):
        first, _, count = trees[tree]
        if not count:
            continue
        for number, (_, possible) in enumerate(ways):
            for source in range(shards):
                level, place = source // across, source % across
                used = (level <= z, level >= z, place <= x, place >= x)[number]
                if first is along_z and number < 2:
                    used = jnp.logical_and(used, place == x)
                if first is along_x and number >= 2:
                    used = jnp.logical_and(used, level == z)

                @pl.when(jnp.logical_and(possible, used))
                def _(tree=tree, number=number, source=source, count=count):
                    piece = gathered.at[rows_of(source), pl.ds(0, count * width)]
                    remote(
                        piece,
                        piece,
                        row_send.at[tree, number, source],
                        row_recv.at[source, 0],
                        "fs",
                        (me + 1) % shards,
                    ).wait_send()


def flush(gathered, mom, second, gathered_hbm, mom_hbm, second_hbm, sem):
    copies = []
    for i, (src, dst) in enumerate(
        ((gathered, gathered_hbm), (mom, mom_hbm), (second, second_hbm))
    ):
        height = src.shape[0] // largest_divisor(src.shape[0] // 16, 8)
        for n in range(src.shape[0] // height):
            rows = pl.ds(n * height, height)
            copies.append(
                pltpu.make_async_copy(src.at[rows], dst.at[0, rows], sem.at[len(copies)])
            )
    for copy in copies:
        copy.start()
    for copy in copies:
        copy.wait()


def per_device(
    groups, shards, grads, counts, weight, mom, second, in_weight, in_bias, out_weight, out_bias
):
    rows, columns = mom.shape[1], mom.shape[2]
    across = max(d for d in range(1, shards + 1) if shards % d == 0 and d * d <= shards)
    depth = shards // across
    planes = groups // CORES
    chunks = largest_divisor(columns // LANES, MOST_CHUNKS)
    cuts = largest_divisor(columns // LANES, MOST_CUTS)
    hbm = pl.BlockSpec(memory_space=pltpu.HBM)
    vmem = pl.BlockSpec(memory_space=pltpu.VMEM)
    held = (2 * shards + 8) * rows * columns
    gathered, new_mom, new_second = pl.pallas_call(
        functools.partial(kernel, groups, depth, across, chunks),
        out_shape=(
            pltpu.VMEM((rows * shards, columns), jnp.bfloat16),
            pltpu.VMEM((rows, columns), jnp.float32),
            pltpu.VMEM((rows, columns), jnp.float32),
        ),
        in_specs=[hbm] * 9,
        out_specs=(vmem, vmem, vmem),
        scratch_shapes=[
            pltpu.SMEM(counts.shape, jnp.int32),
            pltpu.SMEM(in_weight.shape, jnp.float32),
            pltpu.SMEM(in_bias.shape, jnp.float32),
            pltpu.SMEM(out_weight.shape[::-1], jnp.float32),
            pltpu.SMEM(out_bias.shape, jnp.float32),
            pltpu.VMEM((CORES, planes, rows, columns), jnp.bfloat16),
            pltpu.VMEM((rows, columns), jnp.bfloat16),
            pltpu.VMEM((planes, rows, columns), jnp.bfloat16),
            pltpu.VMEM((planes, rows, columns), jnp.bfloat16),
            pltpu.VMEM((planes - 1, rows, columns), jnp.bfloat16),
            pltpu.VMEM((planes - 1, rows, columns), jnp.bfloat16),
            pltpu.VMEM((rows, columns), jnp.float32),
            pltpu.VMEM((shards, 2, LANES), jnp.float32),
            pltpu.SMEM((in_bias.shape[0],), jnp.float32),
            pltpu.SemaphoreType.DMA((5,)),
            pltpu.SemaphoreType.DMA((CORES, planes)),
            pltpu.SemaphoreType.DMA((3,)),
            pltpu.SemaphoreType.DMA((planes, cuts)),
            pltpu.SemaphoreType.DMA((planes, cuts)),
            pltpu.SemaphoreType.DMA((planes - 1, cuts)),
            pltpu.SemaphoreType.DMA((planes - 1, cuts)),
            pltpu.SemaphoreType.REGULAR((2,)),
            pltpu.SemaphoreType.DMA((shards - 1,)),
            pltpu.SemaphoreType.DMA((shards,)),
            pltpu.SemaphoreType.DMA((2, 4, shards)),
            pltpu.SemaphoreType.DMA((shards, chunks)),
        ],
        compiler_params=pltpu.CompilerParams(
            collective_id=0,
            has_side_effects=True,
            vmem_limit_bytes=VMEM_BYTES - held,
        ),
        name="learned_update",
    )(counts, in_weight, in_bias, out_weight.T, out_bias, grads, weight, mom, second)
    return pl.pallas_call(
        flush,
        out_shape=(
            jax.ShapeDtypeStruct((1, rows * shards, columns), jnp.bfloat16),
            jax.ShapeDtypeStruct(mom.shape, jnp.float32),
            jax.ShapeDtypeStruct(second.shape, jnp.float32),
        ),
        in_specs=[vmem] * 3,
        out_specs=(hbm, hbm, hbm),
        scratch_shapes=[pltpu.SemaphoreType.DMA((24,))],
        compiler_params=pltpu.CompilerParams(
            has_side_effects=True, vmem_limit_bytes=FLUSH_BYTES
        ),
        name="flush",
    )(gathered, new_mom, new_second)


def solution(mesh):
    in_specs = (
        P("ep", None, "fs", None),
        P(),
        P("ep", "fs", None),
        P("ep", "fs", None),
        P("ep", "fs", None),
        P(),
        P(),
        P(),
        P(),
    )
    out_specs = (P("ep", None, None), P("ep", "fs", None), P("ep", "fs", None))
    body = functools.partial(per_device, mesh.shape["ep"], mesh.shape["fs"])
    return jax.shard_map(
        body, mesh=mesh, in_specs=in_specs, out_specs=out_specs, check_vma=False
    )
```

```python
import functools

import jax
import jax.numpy as jnp
from jax import lax
from jax.experimental import pallas as pl
from jax.experimental.pallas import tpu as pltpu
from jax.sharding import PartitionSpec as P

MOMENTUM_DECAY = 0.9
SECOND_DECAY = 0.99
NORM_EPS = 1e-06
ROOT_EPS = 1e-08
STEP_SCALE = 0.2
EXP_SCALE = 0.5
LANES = 128
CORES = 2
MOST_CHUNKS = 14
MOST_CUTS = 7
CODE_SCALE = 512.0
CODE_LEAST = 2.0**-126
GO_EARLY = 3
LAG = 3
TURN_LAG = 3
VMEM_BYTES = 67043328
FLUSH_BYTES = 1 << 20


def largest_divisor(number, most):
    return max(d for d in range(1, most + 1) if number % d == 0)


def tile_width(columns, most):
    return LANES * largest_divisor(columns // LANES, most // LANES)


def turned_chunks(depth, across, chunks):
    def load(turned):
        straight = chunks - turned
        on_x = (across - 1) * (depth * straight + turned)
        on_z = (depth - 1) * (straight + across * turned)
        return max(on_x, on_z)

    return min(range(chunks + 1), key=load)


def remote(src, dst, send_sem, recv_sem, axis, peer):
    return pltpu.make_async_remote_copy(
        src_ref=src,
        dst_ref=dst,
        send_sem=send_sem,
        recv_sem=recv_sem,
        device_id={axis: peer},
        device_id_type=pl.DeviceIdType.MESH,
    )


def coded(value):
    power = value * CODE_SCALE
    for _ in range(3):
        power = power * power
    return jnp.where(value < 0.0, -power, power).astype(jnp.bfloat16)


def decoded(code):
    code = code.astype(jnp.float32)
    fourth = lax.rsqrt(lax.rsqrt(jnp.maximum(jnp.abs(code), CODE_LEAST)))
    size = fourth * lax.rsqrt(fourth) * (1.0 / CODE_SCALE)
    return jnp.where(code == 0.0, 0.0, jnp.where(code < 0.0, -size, size))


def signal(semaphore, axis, peer):
    pl.semaphore_signal(
        semaphore, inc=1, device_id={axis: peer}, device_id_type=pl.DeviceIdType.MESH
    )


def kernel(
    groups,
    depth,
    across,
    chunks,
    counts_hbm,
    in_weight_hbm,
    in_bias_hbm,
    out_weight_hbm,
    out_bias_hbm,
    grads_hbm,
    weight_hbm,
    mom_hbm,
    second_hbm,
    gathered,
    mom,
    second,
    counts,
    in_weight,
    in_bias,
    out_weight,
    out_bias,
    grads,
    weight,
    handed,
    taken,
    outgoing,
    arrived,
    gradient,
    sums,
    bias,
    small_sem,
    slab_sem,
    param_sem,
    pair_send,
    pair_recv,
    own_recv,
    grad_send,
    grad_recv,
    chain,
    go,
    sum_sem,
    row_send,
    near_recv,
    turned_recv,
    straight_recv,
):
    shards = depth * across
    planes = groups // CORES
    rows, columns = mom.shape
    units = in_bias.shape[0]
    me_group = lax.axis_index("ep")
    plane = me_group // CORES
    core = me_group % CORES
    partner = plane * CORES + (CORES - 1 - core)
    me = lax.axis_index("fs")
    z = me // across
    x = me % across

    def own_of(step):
        return (plane + step) % planes * CORES + core

    def other_of(step):
        return (plane + step) % planes * CORES + (CORES - 1 - core)

    barrier = pltpu.get_barrier_semaphore()
    signal(barrier, "ep", partner)
    for step in range(1, planes):
        signal(barrier, "ep", own_of(step))
    for step in range(1, across):
        signal(barrier, "fs", z * across + (x + step) % across)

    @pl.when(z < depth - 1)
    def _():
        signal(barrier, "fs", me + across)

    @pl.when(z > 0)
    def _():
        signal(barrier, "fs", me - across)

    small = [
        pltpu.make_async_copy(src, dst, small_sem.at[i])
        for i, (src, dst) in enumerate(
            (
                (counts_hbm, counts),
                (in_weight_hbm, in_weight),
                (in_bias_hbm, in_bias),
                (out_weight_hbm, out_weight),
                (out_bias_hbm, out_bias),
            )
        )
    ]
    for copy in small:
        copy.start()

    order = [*range(1, planes), 0]
    for kind, expert_of in enumerate((other_of, own_of)):
        for step in order:
            pltpu.make_async_copy(
                grads_hbm.at[0, expert_of(step)], grads.at[kind, step], slab_sem.at[kind]
            ).start()

    def await_slabs(kind):
        pltpu.make_async_copy(
            grads_hbm.at[0, pl.ds(0, planes)], grads.at[kind], slab_sem.at[kind]
        ).wait()

    params = [
        pltpu.make_async_copy(src.at[0], dst, param_sem.at[i])
        for i, (src, dst) in enumerate(
            (
                (mom_hbm, mom),
                (second_hbm, second),
                (weight_hbm, weight),
            )
        )
    ]
    for copy in params:
        copy.start()

    cuts = grad_recv.shape[1]
    cut = columns // cuts
    narrow = tile_width(cut, 1024)

    def cols_of(c, i):
        return pl.ds(pl.multiple_of(c * cut + i * narrow, narrow), narrow)

    def piece_of(c):
        return pl.ds(pl.multiple_of(c * cut, cut), cut)

    for copy in small:
        copy.wait()

    def share_of(expert):
        total = counts[0, expert]
        for s in range(1, groups):
            total = total + counts[s, expert]
        mine = jnp.full((1, LANES), counts[me_group, expert].astype(jnp.float32))
        return (mine / jnp.full((1, LANES), total.astype(jnp.float32)))[:, :1]

    shares = [
        [share_of(expert_of(step)) for step in range(planes)] for expert_of in (other_of, own_of)
    ]

    def weighted(kind, step, cols):
        value = shares[kind][step] * grads[kind, step, :, cols].astype(jnp.float32)
        return value.astype(jnp.bfloat16)

    await_slabs(0)

    def hand(i, carry):
        cols = pl.ds(pl.multiple_of(i * narrow, narrow), narrow)
        for step in order:
            handed[step, :, cols] = weighted(0, step, cols)
        return carry

    lax.fori_loop(0, columns // narrow, hand, 0)
    await_slabs(1)

    near = 1 + (planes - 1) + (across - 1)
    near = near + (z > 0).astype(jnp.int32) + (z < depth - 1).astype(jnp.int32)
    pl.semaphore_wait(barrier, near)

    def pair_copy(step, c):
        return remote(
            handed.at[step, :, piece_of(c)],
            taken.at[step, :, piece_of(c)],
            pair_send,
            pair_recv.at[step - 1, c],
            "ep",
            partner,
        )

    own_copy = remote(handed.at[0], taken.at[0], pair_send, own_recv, "ep", partner)

    def grad_copy(step, c):
        return remote(
            outgoing.at[step - 1, :, piece_of(c)],
            arrived.at[step - 1, :, piece_of(c)],
            grad_send,
            grad_recv.at[step - 1, c],
            "ep",
            own_of(step),
        )

    def start_pairs(c, carry):
        for step in order[:-1]:
            pair_copy(step, c).start()
        return carry

    lax.fori_loop(0, cuts, start_pairs, 0)
    own_copy.start()

    def send_piece(c, carry):
        for step in order[:-1]:
            pair_copy(step, c).wait_recv()

            def add(i, inner, step=step):
                cols = cols_of(c, i)
                total = weighted(1, step, cols).astype(jnp.float32)
                total = total + taken[step, :, cols].astype(jnp.float32)
                outgoing[step - 1, :, cols] = coded(total)
                return inner

            lax.fori_loop(0, cut // narrow, add, 0)
            grad_copy(step, c).start()
        return carry

    @pl.when(core == 0)
    def _():
        lax.fori_loop(0, cuts, send_piece, 0)

    def pass_up():
        @pl.when(z > 0)
        def _():
            pl.semaphore_wait(chain.at[0], 1)

        @pl.when(z < depth - 1)
        def _():
            signal(chain.at[0], "fs", me + across)

    def pass_down():
        @pl.when(z < depth - 1)
        def _():
            pl.semaphore_wait(chain.at[1], 1)

        @pl.when(z > 0)
        def _():
            signal(chain.at[1], "fs", me - across)

    @pl.when(z < depth // 2)
    def _():
        pass_up()
        pass_down()

    @pl.when(z >= depth // 2)
    def _():
        pass_down()
        pass_up()

    own_copy.wait_recv()

    def gather_own(i, carry):
        cols = pl.ds(pl.multiple_of(i * narrow, narrow), narrow)
        mine = weighted(1, 0, cols).astype(jnp.float32)
        gradient[:, cols] = mine + taken[0, :, cols].astype(jnp.float32)
        return carry

    lax.fori_loop(0, columns // narrow, gather_own, 0)
    for copy in params:
        copy.wait()

    @pl.when(core > 0)
    def _():
        pl.semaphore_wait(go, 1)
        lax.fori_loop(0, cuts, send_piece, 0)

    def moments(c, carry):
        for step in range(1, planes):
            grad_copy(step, c).wait_recv()

        @pl.when(jnp.logical_and(core == 0, c == max(cuts - GO_EARLY, 0)))
        def _():
            signal(go, "ep", partner)

        def one(i, inner):
            grad_acc, mom_acc = inner
            cols = cols_of(c, i)
            total = gradient[:, cols]
            for step in range(1, planes):
                total = total + decoded(arrived[step - 1, :, cols])
            mom_next = MOMENTUM_DECAY * mom[:, cols] + (1.0 - MOMENTUM_DECAY) * total
            gradient[:, cols] = total
            mom[:, cols] = mom_next
            second[:, cols] = (
                SECOND_DECAY * second[:, cols] + (1.0 - SECOND_DECAY) * total * total
            )
            return grad_acc + total * total, mom_acc + mom_next * mom_next

        return lax.fori_loop(0, cut // narrow, one, carry)

    zero = jnp.zeros((rows, narrow), jnp.float32)
    grad_acc, mom_acc = lax.fori_loop(0, cuts, moments, (zero, zero))

    def to_lanes(acc):
        acc = jnp.sum(acc, axis=0, keepdims=True)
        return sum(acc[:, j : j + LANES] for j in range(0, narrow, LANES))

    sums[me, 0:1, :] = to_lanes(grad_acc)
    sums[me, 1:2, :] = to_lanes(mom_acc)
    for step in range(1, shards):
        remote(
            sums.at[me], sums.at[me], sum_sem.at[0], sum_sem.at[1], "fs", (me + step) % shards
        ).start()
    others = sums.at[pl.ds(0, shards - 1)]
    all_sums = remote(others, others, sum_sem.at[0], sum_sem.at[1], "fs", (me + 1) % shards)
    all_sums.wait_recv()

    entries = rows * columns * shards
    totals = sums[0]
    for s in range(1, shards):
        totals = totals + sums[s]
    mean = jnp.broadcast_to(jnp.sum(totals, axis=1, keepdims=True) / entries, (2, LANES)) + NORM_EPS
    inverse = lax.rsqrt(mean)
    inv_grad = inverse[0:1, :1]
    inv_mom = inverse[1:2, :1]
    log_mom = jnp.max(0.5 * jnp.log(mean[1:2, :]))
    for h in range(units):
        bias[h] = in_bias[h] + in_weight[5, h] * log_mom

    width = columns // chunks
    tile = tile_width(width, 256)

    def learned_step(cols):
        grad = gradient[:, cols]
        mom_next = mom[:, cols]
        old = weight[:, cols].astype(jnp.float32)
        inv_root = lax.rsqrt(second[:, cols] + ROOT_EPS)
        features = (
            grad * inv_grad,
            mom_next * inv_mom,
            mom_next * inv_root,
            grad * inv_root,
            old,
        )
        direction = jnp.full(grad.shape, out_bias[0])
        magnitude = jnp.full(grad.shape, out_bias[1])
        for h in range(units):
            hidden = features[0] * in_weight[0, h] + bias[h]
            for f in range(1, len(features)):
                hidden = hidden + features[f] * in_weight[f, h]
            hidden = jnp.maximum(hidden, 0.0)
            direction = direction + hidden * out_weight[0, h]
            magnitude = magnitude + hidden * out_weight[1, h]
        update = STEP_SCALE * direction * jnp.exp(EXP_SCALE * magnitude)
        return (old - update).astype(jnp.bfloat16)

    def rows_of(source):
        return pl.ds(pl.multiple_of(source * rows, rows), rows)

    ways = (
        (across, z < depth - 1),
        (-across, z > 0),
        (1, x < across - 1),
        (-1, x > 0),
    )
    turned = turned_chunks(depth, across, chunks)
    period = chunks // turned if turned else chunks
    along_z = (z, depth, across, (0, 1))
    along_x = (x, across, 1, (2, 3))
    trees = ((along_x, along_z, turned), (along_z, along_x, chunks - turned))

    def in_tree(tree, k):
        if not turned:
            return k >= 0 if tree else k < 0
        chosen = jnp.logical_and(k % period == period // 2, k // period < turned)
        return jnp.logical_not(chosen) if tree else chosen

    def block(source, k):
        return gathered.at[rows_of(source), pl.ds(pl.multiple_of(k * width, width), width)]

    def far_sem(tree, source, k):
        if trees[tree][1][1] == 2:
            k = 0
        elif not tree:
            k = k // period
        return (turned_recv, straight_recv)[tree].at[source, k]

    def send(tree, source, place, k, which):
        for number in which:
            offset, possible = ways[number]
            near = number in trees[tree][0][3]

            @pl.when(possible)
            def _(number=number, offset=offset, near=near):
                piece = block(source, k)
                remote(
                    piece,
                    piece,
                    row_send.at[tree, number],
                    near_recv.at[place, k] if near else far_sem(tree, source, k),
                    "fs",
                    me + offset,
                ).start()

    def await_near(source, place, k):
        piece = block(source, k)
        remote(
            piece, piece, row_send.at[0, 0], near_recv.at[place, k], "fs", source
        ).wait_recv()

    def await_far(tree, source, k):
        piece = block(source, k)
        remote(
            piece, piece, row_send.at[0, 0], far_sem(tree, source, k), "fs", source
        ).wait_recv()

    def live(tree, k):
        inside = jnp.logical_and(k >= 0, k < chunks)
        return jnp.logical_and(inside, in_tree(tree, jnp.maximum(k, 0)))

    def relay(t, tree):
        first, second, count = trees[tree]
        if not count:
            return
        at, size, stride, (up, down) = first
        other, length, pitch, (up_other, down_other) = second
        lag = LAG if tree else TURN_LAG
        for d in range(size - 1, 0, -1):
            k = t - lag * d

            @pl.when(live(tree, k))
            def _(d=d, k=k):
                @pl.when(at >= d)
                def _():
                    source = me - d * stride
                    await_near(source, at - d, k)
                    send(tree, source, at - d, k, (up,) + second[3])

                @pl.when(at + d < size)
                def _():
                    source = me + d * stride
                    await_near(source, at + d, k)
                    send(tree, source, at + d, k, (down,) + second[3])

        for e in range(length - 2, 0, -1):
            k = t - lag * (size - 1) - LAG * e

            @pl.when(live(tree, k))
            def _(e=e, k=k):
                for level in range(size):

                    @pl.when(jnp.logical_and(other >= e, other < length - 1))
                    def _(level=level):
                        source = level * stride + (other - e) * pitch
                        await_far(tree, source, k)
                        send(tree, source, level, k, (up_other,))

                    @pl.when(jnp.logical_and(other + e < length, other > 0))
                    def _(level=level):
                        source = level * stride + (other + e) * pitch
                        await_far(tree, source, k)
                        send(tree, source, level, k, (down_other,))

    def turn(t, carry):
        @pl.when(t < chunks)
        def _():
            def one(i, inner):
                cols = pl.ds(pl.multiple_of(t * width + i * tile, tile), tile)
                gathered[rows_of(me), cols] = learned_step(cols)
                return inner

            lax.fori_loop(0, width // tile, one, 0)

        for tree in range(2):

            @pl.when(live(tree, t))
            def _(tree=tree):
                send(tree, me, trees[tree][0][0], t, (0, 1, 2, 3))

        for tree in (1, 0):
            relay(t, tree)
        return carry

    reach = max(
        LAG * (depth - 1) + LAG * max(across - 2, 0),
        TURN_LAG * (across - 1) + LAG * max(depth - 2, 0),
    )
    lax.fori_loop(0, chunks + reach, turn, 0)

    def finish(k, carry):
        for tree in range(2):
            first, second, count = trees[tree]
            _, size, stride, _ = first
            other, length, pitch, _ = second
            if length == 2:
                continue

            @pl.when(in_tree(tree, k))
            def _(tree=tree, size=size, stride=stride, other=other, length=length, pitch=pitch):
                for level in range(size):
                    for place in range(length):
                        below = jnp.logical_and(place < other, other == length - 1)
                        above = jnp.logical_and(place > other, other == 0)

                        @pl.when(jnp.logical_or(below, above))
                        def _(level=level, place=place):
                            await_far(tree, level * stride + place * pitch, k)

        return carry

    lax.fori_loop(0, chunks, finish, 0)
    for tree in range(2):
        (at, size, stride, moves), (other, length, pitch, far_moves), count = trees[tree]
        if not count:
            continue
        span = pl.ds(0, count * width)
        if length == 2:
            for level in range(size):
                source = level * stride + (1 - other) * pitch
                piece = gathered.at[rows_of(source), span]
                remote(
                    piece, piece, row_send.at[0, 0], far_sem(tree, source, 0), "fs", source
                ).wait_recv()

        def drain(number, position, extent, going_up, each):
            for p in range(extent - 1):
                here = p if going_up else extent - 1 - p

                @pl.when(position == here)
                def _(p=p):
                    piece = gathered.at[pl.ds(0, (p + 1) * each * rows), span]
                    remote(
                        piece,
                        piece,
                        row_send.at[tree, number],
                        sum_sem.at[1],
                        "fs",
                        (me + 1) % shards,
                    ).wait_send()

        for number, going_up in zip(moves, (True, False)):
            drain(number, at, size, going_up, 1)
        for number, going_up in zip(far_moves, (True, False)):
            drain(number, other, length, going_up, size)

    whole = remote(handed, taken, pair_send, own_recv, "ep", partner)
    whole.wait_send()
    remote(outgoing, arrived, grad_send, own_recv, "ep", partner).wait_send()
    all_sums.wait_send()


def flush(gathered, mom, second, gathered_hbm, mom_hbm, second_hbm, sem):
    pairs = ((gathered, gathered_hbm), (mom, mom_hbm), (second, second_hbm))
    for i, (src, dst) in enumerate(pairs):
        height = src.shape[0] // largest_divisor(src.shape[0] // 16, 8)
        for n in range(src.shape[0] // height):
            rows = pl.ds(n * height, height)
            pltpu.make_async_copy(src.at[rows], dst.at[0, rows], sem.at[i]).start()
    for i, (src, dst) in enumerate(pairs):
        pltpu.make_async_copy(src, dst.at[0], sem.at[i]).wait()


def per_device(
    groups, shards, grads, counts, weight, mom, second, in_weight, in_bias, out_weight, out_bias
):
    rows, columns = mom.shape[1], mom.shape[2]
    across = max(d for d in range(1, shards + 1) if shards % d == 0 and d * d <= shards)
    depth = shards // across
    planes = groups // CORES
    chunks = largest_divisor(columns // LANES, MOST_CHUNKS)
    cuts = largest_divisor(columns // LANES, MOST_CUTS)
    turned = turned_chunks(depth, across, chunks)
    hbm = pl.BlockSpec(memory_space=pltpu.HBM)
    vmem = pl.BlockSpec(memory_space=pltpu.VMEM)
    held = (2 * shards + 8) * rows * columns
    gathered, new_mom, new_second = pl.pallas_call(
        functools.partial(kernel, groups, depth, across, chunks),
        out_shape=(
            pltpu.VMEM((rows * shards, columns), jnp.bfloat16),
            pltpu.VMEM((rows, columns), jnp.float32),
            pltpu.VMEM((rows, columns), jnp.float32),
        ),
        in_specs=[hbm] * 9,
        out_specs=(vmem, vmem, vmem),
        scratch_shapes=[
            pltpu.SMEM(counts.shape, jnp.int32),
            pltpu.SMEM(in_weight.shape, jnp.float32),
            pltpu.SMEM(in_bias.shape, jnp.float32),
            pltpu.SMEM(out_weight.shape[::-1], jnp.float32),
            pltpu.SMEM(out_bias.shape, jnp.float32),
            pltpu.VMEM((CORES, planes, rows, columns), jnp.bfloat16),
            pltpu.VMEM((rows, columns), jnp.bfloat16),
            pltpu.VMEM((planes, rows, columns), jnp.bfloat16),
            pltpu.VMEM((planes, rows, columns), jnp.bfloat16),
            pltpu.VMEM((planes - 1, rows, columns), jnp.bfloat16),
            pltpu.VMEM((planes - 1, rows, columns), jnp.bfloat16),
            pltpu.VMEM((rows, columns), jnp.float32),
            pltpu.VMEM((shards, 2, LANES), jnp.float32),
            pltpu.SMEM((in_bias.shape[0],), jnp.float32),
            pltpu.SemaphoreType.DMA((5,)),
            pltpu.SemaphoreType.DMA((CORES,)),
            pltpu.SemaphoreType.DMA((3,)),
            pltpu.SemaphoreType.DMA,
            pltpu.SemaphoreType.DMA((planes - 1, cuts)),
            pltpu.SemaphoreType.DMA,
            pltpu.SemaphoreType.DMA,
            pltpu.SemaphoreType.DMA((planes - 1, cuts)),
            pltpu.SemaphoreType.REGULAR((2,)),
            pltpu.SemaphoreType.REGULAR,
            pltpu.SemaphoreType.DMA((2,)),
            pltpu.SemaphoreType.DMA((2, 4)),
            pltpu.SemaphoreType.DMA((max(depth, across), chunks)),
            pltpu.SemaphoreType.DMA((shards, 1 if depth == 2 else max(turned, 1))),
            pltpu.SemaphoreType.DMA((shards, 1 if across == 2 else chunks)),
        ],
        compiler_params=pltpu.CompilerParams(
            collective_id=0,
            has_side_effects=True,
            vmem_limit_bytes=VMEM_BYTES - held,
        ),
        name="learned_update",
    )(counts, in_weight, in_bias, out_weight.T, out_bias, grads, weight, mom, second)
    return pl.pallas_call(
        flush,
        out_shape=(
            jax.ShapeDtypeStruct((1, rows * shards, columns), jnp.bfloat16),
            jax.ShapeDtypeStruct(mom.shape, jnp.float32),
            jax.ShapeDtypeStruct(second.shape, jnp.float32),
        ),
        in_specs=[vmem] * 3,
        out_specs=(hbm, hbm, hbm),
        scratch_shapes=[pltpu.SemaphoreType.DMA((3,))],
        compiler_params=pltpu.CompilerParams(
            has_side_effects=True, vmem_limit_bytes=FLUSH_BYTES
        ),
        name="flush",
    )(gathered, new_mom, new_second)


def solution(mesh):
    in_specs = (
        P("ep", None, "fs", None),
        P(),
        P("ep", "fs", None),
        P("ep", "fs", None),
        P("ep", "fs", None),
        P(),
        P(),
        P(),
        P(),
    )
    out_specs = (P("ep", None, None), P("ep", "fs", None), P("ep", "fs", None))
    body = functools.partial(per_device, mesh.shape["ep"], mesh.shape["fs"])
    return jax.shard_map(
        body, mesh=mesh, in_specs=in_specs, out_specs=out_specs, check_vma=False
    )
```

```python
import functools

import jax
import jax.numpy as jnp
from jax import lax
from jax.experimental import pallas as pl
from jax.experimental.pallas import tpu as pltpu
from jax.sharding import PartitionSpec as P

MOMENTUM_DECAY = 0.9
SECOND_DECAY = 0.99
NORM_EPS = 1e-06
ROOT_EPS = 1e-08
STEP_SCALE = 0.2
EXP_SCALE = 0.5
LANES = 128
CORES = 2
MOST_CHUNKS = 14
MOST_CUTS = 7
CODE_SCALE = 512.0
CODE_LEAST = 2.0**-126
GO_EARLY = 3
LAG = 2
TURN_LAG = 3
VMEM_BYTES = 67043328
FLUSH_BYTES = 1 << 20
TERMS = 16
MOST_TILE = 1024


def largest_divisor(number, most):
    return max(d for d in range(1, most + 1) if number % d == 0)


def tile_width(columns, most):
    return LANES * largest_divisor(columns // LANES, most // LANES)


def turned_chunks(depth, across, chunks):
    def load(turned):
        straight = chunks - turned
        on_x = (across - 1) * (depth * straight + turned)
        on_z = (depth - 1) * (straight + across * turned)
        return max(on_x, on_z)

    return min(range(chunks + 1), key=load)


def remote(src, dst, send_sem, recv_sem, axis, peer):
    return pltpu.make_async_remote_copy(
        src_ref=src,
        dst_ref=dst,
        send_sem=send_sem,
        recv_sem=recv_sem,
        device_id={axis: peer},
        device_id_type=pl.DeviceIdType.MESH,
    )


def coded(value):
    power = value * CODE_SCALE
    for _ in range(3):
        power = power * power
    return jnp.where(value < 0.0, -power, power).astype(jnp.bfloat16)


def decoded(code):
    code = code.astype(jnp.float32)
    fourth = lax.rsqrt(lax.rsqrt(jnp.maximum(jnp.abs(code), CODE_LEAST)))
    size = fourth * lax.rsqrt(fourth) * (1.0 / CODE_SCALE)
    return jnp.where(code == 0.0, 0.0, jnp.where(code < 0.0, -size, size))


def signal(semaphore, axis, peer):
    pl.semaphore_signal(
        semaphore, inc=1, device_id={axis: peer}, device_id_type=pl.DeviceIdType.MESH
    )


def kernel(
    groups,
    depth,
    across,
    chunks,
    counts_hbm,
    in_weight_hbm,
    in_bias_hbm,
    out_weight_hbm,
    out_bias_hbm,
    grads_hbm,
    weight_hbm,
    mom_hbm,
    second_hbm,
    gathered,
    mom,
    second,
    counts,
    in_weight,
    in_bias,
    out_weight,
    out_bias,
    grads,
    weight,
    handed,
    taken,
    outgoing,
    arrived,
    gradient,
    sums,
    layer,
    floor,
    small_sem,
    slab_sem,
    param_sem,
    pair_send,
    pair_recv,
    own_recv,
    grad_send,
    grad_recv,
    chain,
    go,
    sum_sem,
    row_send,
    near_recv,
    turned_recv,
    straight_recv,
):
    shards = depth * across
    planes = groups // CORES
    rows, columns = mom.shape
    units = in_bias.shape[0]
    me_group = lax.axis_index("ep")
    plane = me_group // CORES
    core = me_group % CORES
    partner = plane * CORES + (CORES - 1 - core)
    me = lax.axis_index("fs")
    z = me // across
    x = me % across

    def own_of(step):
        return (plane + step) % planes * CORES + core

    def other_of(step):
        return (plane + step) % planes * CORES + (CORES - 1 - core)

    barrier = pltpu.get_barrier_semaphore()
    signal(barrier, "ep", partner)
    for step in range(1, planes):
        signal(barrier, "ep", own_of(step))
    for step in range(1, across):
        signal(barrier, "fs", z * across + (x + step) % across)

    @pl.when(z < depth - 1)
    def _():
        signal(barrier, "fs", me + across)

    @pl.when(z > 0)
    def _():
        signal(barrier, "fs", me - across)

    small = [
        pltpu.make_async_copy(src, dst, small_sem.at[i])
        for i, (src, dst) in enumerate(
            (
                (counts_hbm, counts),
                (in_weight_hbm, in_weight),
                (in_bias_hbm, in_bias),
                (out_weight_hbm, out_weight),
                (out_bias_hbm, out_bias),
            )
        )
    ]
    for copy in small:
        copy.start()

    order = [*range(1, planes), 0]
    for kind, expert_of in enumerate((other_of, own_of)):
        for step in order:
            pltpu.make_async_copy(
                grads_hbm.at[0, expert_of(step)], grads.at[kind, step], slab_sem.at[kind]
            ).start()

    def await_slabs(kind):
        pltpu.make_async_copy(
            grads_hbm.at[0, pl.ds(0, planes)], grads.at[kind], slab_sem.at[kind]
        ).wait()

    params = [
        pltpu.make_async_copy(src.at[0], dst, param_sem.at[i])
        for i, (src, dst) in enumerate(
            (
                (mom_hbm, mom),
                (second_hbm, second),
                (weight_hbm, weight),
            )
        )
    ]
    for copy in params:
        copy.start()

    cuts = grad_recv.shape[1]
    cut = columns // cuts
    narrow = tile_width(cut, 1024)

    def cols_of(c, i):
        return pl.ds(pl.multiple_of(c * cut + i * narrow, narrow), narrow)

    def piece_of(c):
        return pl.ds(pl.multiple_of(c * cut, cut), cut)

    for copy in small:
        copy.wait()

    def share_of(expert):
        total = counts[0, expert]
        for s in range(1, groups):
            total = total + counts[s, expert]
        mine = jnp.full((1, LANES), counts[me_group, expert].astype(jnp.float32))
        return (mine / jnp.full((1, LANES), total.astype(jnp.float32)))[:, :1]

    shares = [
        [share_of(expert_of(step)) for step in range(planes)] for expert_of in (other_of, own_of)
    ]

    def weighted(kind, step, cols):
        value = shares[kind][step] * grads[kind, step, :, cols].astype(jnp.float32)
        return value.astype(jnp.bfloat16)

    await_slabs(0)

    def hand(i, carry):
        cols = pl.ds(pl.multiple_of(i * narrow, narrow), narrow)
        for step in order:
            handed[step, :, cols] = weighted(0, step, cols)
        return carry

    lax.fori_loop(0, columns // narrow, hand, 0)
    await_slabs(1)

    near = 1 + (planes - 1) + (across - 1)
    near = near + (z > 0).astype(jnp.int32) + (z < depth - 1).astype(jnp.int32)
    pl.semaphore_wait(barrier, near)

    def pair_copy(step, c):
        return remote(
            handed.at[step, :, piece_of(c)],
            taken.at[step, :, piece_of(c)],
            pair_send,
            pair_recv.at[step - 1, c],
            "ep",
            partner,
        )

    own_copy = remote(handed.at[0], taken.at[0], pair_send, own_recv, "ep", partner)

    def grad_copy(step, c):
        return remote(
            outgoing.at[step - 1, :, piece_of(c)],
            arrived.at[step - 1, :, piece_of(c)],
            grad_send,
            grad_recv.at[step - 1, c],
            "ep",
            own_of(step),
        )

    def start_pairs(c, carry):
        for step in order[:-1]:
            pair_copy(step, c).start()
        return carry

    lax.fori_loop(0, cuts, start_pairs, 0)
    own_copy.start()

    def send_piece(c, carry):
        for step in order[:-1]:
            pair_copy(step, c).wait_recv()

            def add(i, inner, step=step):
                cols = cols_of(c, i)
                total = weighted(1, step, cols).astype(jnp.float32)
                total = total + taken[step, :, cols].astype(jnp.float32)
                outgoing[step - 1, :, cols] = coded(total)
                return inner

            lax.fori_loop(0, cut // narrow, add, 0)
            grad_copy(step, c).start()
        return carry

    @pl.when(core == 0)
    def _():
        lax.fori_loop(0, cuts, send_piece, 0)

    def pass_up():
        @pl.when(z > 0)
        def _():
            pl.semaphore_wait(chain.at[0], 1)

        @pl.when(z < depth - 1)
        def _():
            signal(chain.at[0], "fs", me + across)

    def pass_down():
        @pl.when(z < depth - 1)
        def _():
            pl.semaphore_wait(chain.at[1], 1)

        @pl.when(z > 0)
        def _():
            signal(chain.at[1], "fs", me - across)

    @pl.when(z < depth // 2)
    def _():
        pass_up()
        pass_down()

    @pl.when(z >= depth // 2)
    def _():
        pass_down()
        pass_up()

    own_copy.wait_recv()

    def gather_own(i, carry):
        cols = pl.ds(pl.multiple_of(i * narrow, narrow), narrow)
        mine = weighted(1, 0, cols).astype(jnp.float32)
        gradient[:, cols] = mine + taken[0, :, cols].astype(jnp.float32)
        return carry

    lax.fori_loop(0, columns // narrow, gather_own, 0)
    for copy in params:
        copy.wait()

    span = layer.shape[1]
    lane = lax.broadcasted_iota(jnp.int32, (rows, span), 1)
    term = lane // rows
    inside = lane % rows == lax.broadcasted_iota(jnp.int32, (rows, span), 0)

    def lay(h, carry):
        high = jnp.zeros((rows, span), jnp.float32)
        low = high
        for f in range(5):
            value = jnp.full((rows, span), in_weight[f, h])
            upper = value.astype(jnp.bfloat16).astype(jnp.float32)
            at_high = term == f
            if f < 4:
                at_high = jnp.logical_or(at_high, term == 5 + f)
            high = jnp.where(at_high, upper, high)
            low = jnp.where(term == 9 + f, value - upper, low)
        block = jnp.where(inside, high + low, 0.0)
        layer[pl.ds(pl.multiple_of(h * rows, rows), rows), :] = block.astype(jnp.bfloat16)
        return carry

    lax.fori_loop(0, units, lay, 0)

    @pl.when(core > 0)
    def _():
        pl.semaphore_wait(go, 1)
        lax.fori_loop(0, cuts, send_piece, 0)

    def moments(c, carry):
        for step in range(1, planes):
            grad_copy(step, c).wait_recv()

        @pl.when(jnp.logical_and(core == 0, c == max(cuts - GO_EARLY, 0)))
        def _():
            signal(go, "ep", partner)

        def one(i, inner):
            grad_acc, mom_acc = inner
            cols = cols_of(c, i)
            total = gradient[:, cols]
            for step in range(1, planes):
                total = total + decoded(arrived[step - 1, :, cols])
            mom_next = MOMENTUM_DECAY * mom[:, cols] + (1.0 - MOMENTUM_DECAY) * total
            gradient[:, cols] = total
            mom[:, cols] = mom_next
            second[:, cols] = (
                SECOND_DECAY * second[:, cols] + (1.0 - SECOND_DECAY) * total * total
            )
            return grad_acc + total * total, mom_acc + mom_next * mom_next

        return lax.fori_loop(0, cut // narrow, one, carry)

    zero = jnp.zeros((rows, narrow), jnp.float32)
    grad_acc, mom_acc = lax.fori_loop(0, cuts, moments, (zero, zero))

    def to_lanes(acc):
        acc = jnp.sum(acc, axis=0, keepdims=True)
        return sum(acc[:, j : j + LANES] for j in range(0, narrow, LANES))

    sums[me, 0:1, :] = to_lanes(grad_acc)
    sums[me, 1:2, :] = to_lanes(mom_acc)
    for step in range(1, shards):
        remote(
            sums.at[me], sums.at[me], sum_sem.at[0], sum_sem.at[1], "fs", (me + step) % shards
        ).start()
    others = sums.at[pl.ds(0, shards - 1)]
    all_sums = remote(others, others, sum_sem.at[0], sum_sem.at[1], "fs", (me + 1) % shards)
    all_sums.wait_recv()

    entries = rows * columns * shards
    totals = sums[0]
    for s in range(1, shards):
        totals = totals + sums[s]
    mean = jnp.broadcast_to(jnp.sum(totals, axis=1, keepdims=True) / entries, (2, LANES)) + NORM_EPS
    inverse = lax.rsqrt(mean)
    inv_grad = inverse[0:1, :1]
    inv_mom = inverse[1:2, :1]
    log_mom = jnp.max(0.5 * jnp.log(mean[1:2, :]))
    starts = [out_bias[0], out_bias[1]]
    for h in range(units):
        bias = in_bias[h] + in_weight[5, h] * log_mom
        floor[h] = -bias
        for i in range(2):
            starts[i] = starts[i] + bias * out_weight[i, h]

    width = columns // chunks
    tile = tile_width(width, MOST_TILE)

    def learned_step(cols):
        grad = gradient[:, cols]
        mom_next = mom[:, cols]
        old = weight[:, cols]
        inv_root = lax.rsqrt(second[:, cols] + ROOT_EPS)
        features = (
            grad * inv_grad,
            mom_next * inv_mom,
            mom_next * inv_root,
            grad * inv_root,
        )
        high = [feature.astype(jnp.bfloat16) for feature in features]
        low = [
            (feature - part.astype(jnp.float32)).astype(jnp.bfloat16)
            for feature, part in zip(features, high)
        ]
        terms = [*high, old, *low, *high, old]
        terms = terms + [jnp.zeros_like(old)] * (TERMS - len(terms))
        hidden = jnp.dot(
            layer[...], jnp.concatenate(terms, axis=0), preferred_element_type=jnp.float32
        )
        direction = jnp.full(grad.shape, starts[0])
        magnitude = jnp.full(grad.shape, starts[1])
        for h in range(units):
            above = jnp.maximum(hidden[h * rows : (h + 1) * rows], floor[h])
            direction = direction + above * out_weight[0, h]
            magnitude = magnitude + above * out_weight[1, h]
        update = STEP_SCALE * direction * jnp.exp(EXP_SCALE * magnitude)
        return (old.astype(jnp.float32) - update).astype(jnp.bfloat16)

    def rows_of(source):
        return pl.ds(pl.multiple_of(source * rows, rows), rows)

    ways = (
        (across, z < depth - 1),
        (-across, z > 0),
        (1, x < across - 1),
        (-1, x > 0),
    )
    turned = turned_chunks(depth, across, chunks)
    period = chunks // turned if turned else chunks
    along_z = (z, depth, across, (0, 1))
    along_x = (x, across, 1, (2, 3))
    trees = ((along_x, along_z, turned), (along_z, along_x, chunks - turned))

    def in_tree(tree, k):
        if not turned:
            return k >= 0 if tree else k < 0
        chosen = jnp.logical_and(k % period == period // 2, k // period < turned)
        return jnp.logical_not(chosen) if tree else chosen

    def block(source, k):
        return gathered.at[rows_of(source), pl.ds(pl.multiple_of(k * width, width), width)]

    def far_sem(tree, source, k):
        if trees[tree][1][1] == 2:
            k = 0
        elif not tree:
            k = k // period
        return (turned_recv, straight_recv)[tree].at[source, k]

    def send(tree, source, place, k, which):
        for number in which:
            offset, possible = ways[number]
            near = number in trees[tree][0][3]

            @pl.when(possible)
            def _(number=number, offset=offset, near=near):
                piece = block(source, k)
                remote(
                    piece,
                    piece,
                    row_send.at[tree, number],
                    near_recv.at[place, k] if near else far_sem(tree, source, k),
                    "fs",
                    me + offset,
                ).start()

    def await_near(source, place, k):
        piece = block(source, k)
        remote(
            piece, piece, row_send.at[0, 0], near_recv.at[place, k], "fs", source
        ).wait_recv()

    def await_far(tree, source, k):
        piece = block(source, k)
        remote(
            piece, piece, row_send.at[0, 0], far_sem(tree, source, k), "fs", source
        ).wait_recv()

    def live(tree, k):
        inside = jnp.logical_and(k >= 0, k < chunks)
        return jnp.logical_and(inside, in_tree(tree, jnp.maximum(k, 0)))

    def relay(t, tree):
        first, second, count = trees[tree]
        if not count:
            return
        at, size, stride, (up, down) = first
        other, length, pitch, (up_other, down_other) = second
        lag = LAG if tree else TURN_LAG
        for d in range(size - 1, 0, -1):
            k = t - lag * d

            @pl.when(live(tree, k))
            def _(d=d, k=k):
                @pl.when(at >= d)
                def _():
                    source = me - d * stride
                    await_near(source, at - d, k)
                    send(tree, source, at - d, k, (up,) + second[3])

                @pl.when(at + d < size)
                def _():
                    source = me + d * stride
                    await_near(source, at + d, k)
                    send(tree, source, at + d, k, (down,) + second[3])

        for e in range(length - 2, 0, -1):
            k = t - lag * (size - 1) - LAG * e

            @pl.when(live(tree, k))
            def _(e=e, k=k):
                for level in range(size):

                    @pl.when(jnp.logical_and(other >= e, other < length - 1))
                    def _(level=level):
                        source = level * stride + (other - e) * pitch
                        await_far(tree, source, k)
                        send(tree, source, level, k, (up_other,))

                    @pl.when(jnp.logical_and(other + e < length, other > 0))
                    def _(level=level):
                        source = level * stride + (other + e) * pitch
                        await_far(tree, source, k)
                        send(tree, source, level, k, (down_other,))

    def turn(t, carry):
        @pl.when(t < chunks)
        def _():
            def one(i, inner):
                cols = pl.ds(pl.multiple_of(t * width + i * tile, tile), tile)
                gathered[rows_of(me), cols] = learned_step(cols)
                return inner

            lax.fori_loop(0, width // tile, one, 0)

        for tree in range(2):

            @pl.when(live(tree, t))
            def _(tree=tree):
                send(tree, me, trees[tree][0][0], t, (0, 1, 2, 3))

        for tree in (1, 0):
            relay(t, tree)
        return carry

    reach = max(
        LAG * (depth - 1) + LAG * max(across - 2, 0),
        TURN_LAG * (across - 1) + LAG * max(depth - 2, 0),
    )
    lax.fori_loop(0, chunks + reach, turn, 0)

    def finish(k, carry):
        for tree in range(2):
            first, second, count = trees[tree]
            _, size, stride, _ = first
            other, length, pitch, _ = second
            if length == 2:
                continue

            @pl.when(in_tree(tree, k))
            def _(tree=tree, size=size, stride=stride, other=other, length=length, pitch=pitch):
                for level in range(size):
                    for place in range(length):
                        below = jnp.logical_and(place < other, other == length - 1)
                        above = jnp.logical_and(place > other, other == 0)

                        @pl.when(jnp.logical_or(below, above))
                        def _(level=level, place=place):
                            await_far(tree, level * stride + place * pitch, k)

        return carry

    lax.fori_loop(0, chunks, finish, 0)
    for tree in range(2):
        (at, size, stride, moves), (other, length, pitch, far_moves), count = trees[tree]
        if not count:
            continue
        span = pl.ds(0, count * width)
        if length == 2:
            for level in range(size):
                source = level * stride + (1 - other) * pitch
                piece = gathered.at[rows_of(source), span]
                remote(
                    piece, piece, row_send.at[0, 0], far_sem(tree, source, 0), "fs", source
                ).wait_recv()

        def drain(number, position, extent, going_up, each):
            for p in range(extent - 1):
                here = p if going_up else extent - 1 - p

                @pl.when(position == here)
                def _(p=p):
                    piece = gathered.at[pl.ds(0, (p + 1) * each * rows), span]
                    remote(
                        piece,
                        piece,
                        row_send.at[tree, number],
                        sum_sem.at[1],
                        "fs",
                        (me + 1) % shards,
                    ).wait_send()

        for number, going_up in zip(moves, (True, False)):
            drain(number, at, size, going_up, 1)
        for number, going_up in zip(far_moves, (True, False)):
            drain(number, other, length, going_up, size)

    whole = remote(handed, taken, pair_send, own_recv, "ep", partner)
    whole.wait_send()
    remote(outgoing, arrived, grad_send, own_recv, "ep", partner).wait_send()
    all_sums.wait_send()


def flush(gathered, mom, second, gathered_hbm, mom_hbm, second_hbm, sem):
    pairs = ((gathered, gathered_hbm), (mom, mom_hbm), (second, second_hbm))
    for i, (src, dst) in enumerate(pairs):
        height = src.shape[0] // largest_divisor(src.shape[0] // 16, 8)
        for n in range(src.shape[0] // height):
            rows = pl.ds(n * height, height)
            pltpu.make_async_copy(src.at[rows], dst.at[0, rows], sem.at[i]).start()
    for i, (src, dst) in enumerate(pairs):
        pltpu.make_async_copy(src, dst.at[0], sem.at[i]).wait()


def per_device(
    groups, shards, grads, counts, weight, mom, second, in_weight, in_bias, out_weight, out_bias
):
    rows, columns = mom.shape[1], mom.shape[2]
    across = max(d for d in range(1, shards + 1) if shards % d == 0 and d * d <= shards)
    depth = shards // across
    planes = groups // CORES
    chunks = largest_divisor(columns // LANES, MOST_CHUNKS)
    cuts = largest_divisor(columns // LANES, MOST_CUTS)
    turned = turned_chunks(depth, across, chunks)
    hbm = pl.BlockSpec(memory_space=pltpu.HBM)
    vmem = pl.BlockSpec(memory_space=pltpu.VMEM)
    held = (2 * shards + 8) * rows * columns
    gathered, new_mom, new_second = pl.pallas_call(
        functools.partial(kernel, groups, depth, across, chunks),
        out_shape=(
            pltpu.VMEM((rows * shards, columns), jnp.bfloat16),
            pltpu.VMEM((rows, columns), jnp.float32),
            pltpu.VMEM((rows, columns), jnp.float32),
        ),
        in_specs=[hbm] * 9,
        out_specs=(vmem, vmem, vmem),
        scratch_shapes=[
            pltpu.SMEM(counts.shape, jnp.int32),
            pltpu.SMEM(in_weight.shape, jnp.float32),
            pltpu.SMEM(in_bias.shape, jnp.float32),
            pltpu.SMEM(out_weight.shape[::-1], jnp.float32),
            pltpu.SMEM(out_bias.shape, jnp.float32),
            pltpu.VMEM((CORES, planes, rows, columns), jnp.bfloat16),
            pltpu.VMEM((rows, columns), jnp.bfloat16),
            pltpu.VMEM((planes, rows, columns), jnp.bfloat16),
            pltpu.VMEM((planes, rows, columns), jnp.bfloat16),
            pltpu.VMEM((planes - 1, rows, columns), jnp.bfloat16),
            pltpu.VMEM((planes - 1, rows, columns), jnp.bfloat16),
            pltpu.VMEM((rows, columns), jnp.float32),
            pltpu.VMEM((shards, 2, LANES), jnp.float32),
            pltpu.VMEM((in_bias.shape[0] * rows, TERMS * rows), jnp.bfloat16),
            pltpu.SMEM((in_bias.shape[0],), jnp.float32),
            pltpu.SemaphoreType.DMA((5,)),
            pltpu.SemaphoreType.DMA((CORES,)),
            pltpu.SemaphoreType.DMA((3,)),
            pltpu.SemaphoreType.DMA,
            pltpu.SemaphoreType.DMA((planes - 1, cuts)),
            pltpu.SemaphoreType.DMA,
            pltpu.SemaphoreType.DMA,
            pltpu.SemaphoreType.DMA((planes - 1, cuts)),
            pltpu.SemaphoreType.REGULAR((2,)),
            pltpu.SemaphoreType.REGULAR,
            pltpu.SemaphoreType.DMA((2,)),
            pltpu.SemaphoreType.DMA((2, 4)),
            pltpu.SemaphoreType.DMA((max(depth, across), chunks)),
            pltpu.SemaphoreType.DMA((shards, 1 if depth == 2 else max(turned, 1))),
            pltpu.SemaphoreType.DMA((shards, 1 if across == 2 else chunks)),
        ],
        compiler_params=pltpu.CompilerParams(
            collective_id=0,
            has_side_effects=True,
            vmem_limit_bytes=VMEM_BYTES - held,
        ),
        name="learned_update",
    )(counts, in_weight, in_bias, out_weight.T, out_bias, grads, weight, mom, second)
    return pl.pallas_call(
        flush,
        out_shape=(
            jax.ShapeDtypeStruct((1, rows * shards, columns), jnp.bfloat16),
            jax.ShapeDtypeStruct(mom.shape, jnp.float32),
            jax.ShapeDtypeStruct(second.shape, jnp.float32),
        ),
        in_specs=[vmem] * 3,
        out_specs=(hbm, hbm, hbm),
        scratch_shapes=[pltpu.SemaphoreType.DMA((3,))],
        compiler_params=pltpu.CompilerParams(
            has_side_effects=True, vmem_limit_bytes=FLUSH_BYTES
        ),
        name="flush",
    )(gathered, new_mom, new_second)


def solution(mesh):
    in_specs = (
        P("ep", None, "fs", None),
        P(),
        P("ep", "fs", None),
        P("ep", "fs", None),
        P("ep", "fs", None),
        P(),
        P(),
        P(),
        P(),
    )
    out_specs = (P("ep", None, None), P("ep", "fs", None), P("ep", "fs", None))
    body = functools.partial(per_device, mesh.shape["ep"], mesh.shape["fs"])
    return jax.shard_map(
        body, mesh=mesh, in_specs=in_specs, out_specs=out_specs, check_vma=False
    )
```

```python
import functools

import jax
import jax.numpy as jnp
from jax import lax
from jax.experimental import pallas as pl
from jax.experimental.pallas import tpu as pltpu
from jax.sharding import PartitionSpec as P

MOMENTUM_DECAY = 0.9
SECOND_DECAY = 0.99
NORM_EPS = 1e-06
ROOT_EPS = 1e-08
STEP_SCALE = 0.2
EXP_SCALE = 0.5
LANES = 128
SUBLANES = 8
CORES = 2
MOST_CHUNKS = 14
MOST_CUTS = 7
CODE_SCALE = 512.0
CODE_LEAST = 2.0**-126
GO_EARLY = 3
NEAR_LAGS = (4, 8, 10)
TURN_LAG = 8
FAR_LAGS = (6, 10)
VMEM_BYTES = 67043328
FLUSH_BYTES = 1 << 20
TERMS = 16
MOST_TILE = 1024


def largest_divisor(number, most):
    return max(d for d in range(1, most + 1) if number % d == 0)


def tile_width(columns, most):
    return LANES * largest_divisor(columns // LANES, most // LANES)


def turned_chunks(depth, across, chunks):
    def load(turned):
        straight = chunks - turned
        on_x = (across - 1) * (depth * straight + turned)
        on_z = (depth - 1) * (straight + across * turned)
        return max(on_x, on_z)

    return min(range(chunks + 1), key=load)


def nth(lags, d):
    return lags[d - 1] if d <= len(lags) else lags[-1] * d


def remote(src, dst, send_sem, recv_sem, axis, peer):
    return pltpu.make_async_remote_copy(
        src_ref=src,
        dst_ref=dst,
        send_sem=send_sem,
        recv_sem=recv_sem,
        device_id={axis: peer},
        device_id_type=pl.DeviceIdType.MESH,
    )


def coded(value):
    power = value * CODE_SCALE
    for _ in range(3):
        power = power * power
    return jnp.where(value < 0.0, -power, power).astype(jnp.bfloat16)


def decoded(code):
    code = code.astype(jnp.float32)
    fourth = lax.rsqrt(lax.rsqrt(jnp.maximum(jnp.abs(code), CODE_LEAST)))
    size = fourth * lax.rsqrt(fourth) * (1.0 / CODE_SCALE)
    return jnp.where(code == 0.0, 0.0, jnp.where(code < 0.0, -size, size))


def folded(value):
    rows, columns = value.shape
    parts = [
        value[i : i + SUBLANES, j : j + LANES]
        for i in range(0, rows, SUBLANES)
        for j in range(0, columns, LANES)
    ]
    while len(parts) > 1:
        parts = [a + b for a, b in zip(parts[::2], parts[1::2])] + parts[len(parts) & ~1 :]
    return parts[0]


def signal(semaphore, axis, peer):
    pl.semaphore_signal(
        semaphore, inc=1, device_id={axis: peer}, device_id_type=pl.DeviceIdType.MESH
    )


def kernel(
    groups,
    depth,
    across,
    chunks,
    counts_hbm,
    in_weight_hbm,
    in_bias_hbm,
    out_weight_hbm,
    out_bias_hbm,
    grads_hbm,
    weight_hbm,
    mom_hbm,
    second_hbm,
    gathered,
    mom,
    second,
    counts,
    in_weight,
    in_bias,
    out_weight,
    out_bias,
    grads,
    weight,
    handed,
    taken,
    outgoing,
    arrived,
    gradient,
    sums,
    layer,
    small_sem,
    slab_sem,
    param_sem,
    pair_send,
    pair_recv,
    own_recv,
    grad_send,
    grad_recv,
    chain,
    go,
    sum_sem,
    row_send,
    near_recv,
    turned_recv,
    straight_recv,
):
    shards = depth * across
    planes = groups // CORES
    rows, columns = mom.shape
    units = in_bias.shape[0]
    me_group = lax.axis_index("ep")
    plane = me_group // CORES
    core = me_group % CORES
    partner = plane * CORES + (CORES - 1 - core)
    me = lax.axis_index("fs")
    z = me // across
    x = me % across

    def own_of(step):
        return (plane + step) % planes * CORES + core

    def other_of(step):
        return (plane + step) % planes * CORES + (CORES - 1 - core)

    barrier = pltpu.get_barrier_semaphore()
    signal(barrier, "ep", partner)
    for step in range(1, planes):
        signal(barrier, "ep", own_of(step))
    for step in range(1, across):
        signal(barrier, "fs", z * across + (x + step) % across)

    @pl.when(z < depth - 1)
    def _():
        signal(barrier, "fs", me + across)

    @pl.when(z > 0)
    def _():
        signal(barrier, "fs", me - across)

    small = [
        pltpu.make_async_copy(src, dst, small_sem.at[i])
        for i, (src, dst) in enumerate(
            (
                (counts_hbm, counts),
                (in_weight_hbm, in_weight),
                (in_bias_hbm, in_bias),
                (out_weight_hbm, out_weight),
                (out_bias_hbm, out_bias),
            )
        )
    ]
    def start_slab(kind, step):
        expert = (other_of, own_of)[kind](step)
        sem = slab_sem.at[kind if step else CORES]
        pltpu.make_async_copy(grads_hbm.at[0, expert], grads.at[kind, step], sem).start()

    def await_slabs(kind):
        pltpu.make_async_copy(
            grads_hbm.at[0, pl.ds(0, planes - 1)],
            grads.at[kind, pl.ds(1, planes - 1)],
            slab_sem.at[kind],
        ).wait()

    small[0].start()
    for kind in range(CORES):
        for step in range(1, planes):
            start_slab(kind, step)
    params = [
        pltpu.make_async_copy(src.at[0], dst, param_sem.at[i])
        for i, (src, dst) in enumerate(
            (
                (mom_hbm, mom),
                (second_hbm, second),
                (weight_hbm, weight),
            )
        )
    ]

    cuts = grad_recv.shape[1]
    cut = columns // cuts
    narrow = tile_width(cut, 1024)

    def cols_of(c, i):
        return pl.ds(pl.multiple_of(c * cut + i * narrow, narrow), narrow)

    def piece_of(c):
        return pl.ds(pl.multiple_of(c * cut, cut), cut)

    small[0].wait()

    def share_of(expert):
        total = counts[0, expert]
        for s in range(1, groups):
            total = total + counts[s, expert]
        mine = jnp.full((1, LANES), counts[me_group, expert].astype(jnp.float32))
        return (mine / jnp.full((1, LANES), total.astype(jnp.float32)))[:, :1]

    shares = [
        [share_of(expert_of(step)) for step in range(planes)] for expert_of in (other_of, own_of)
    ]

    def weighted(kind, step, cols):
        value = shares[kind][step] * grads[kind, step, :, cols].astype(jnp.float32)
        return value.astype(jnp.bfloat16)

    near = 1 + (planes - 1) + (across - 1)
    near = near + (z > 0).astype(jnp.int32) + (z < depth - 1).astype(jnp.int32)
    pl.semaphore_wait(barrier, near)

    def pair_copy(step, c):
        return remote(
            handed.at[step, :, piece_of(c)],
            taken.at[step, :, piece_of(c)],
            pair_send,
            pair_recv.at[step - 1, c],
            "ep",
            partner,
        )

    own_copy = remote(handed.at[0], taken.at[0], pair_send, own_recv, "ep", partner)

    def grad_copy(step, c):
        return remote(
            outgoing.at[step - 1, :, piece_of(c)],
            arrived.at[step - 1, :, piece_of(c)],
            grad_send,
            grad_recv.at[step - 1, c],
            "ep",
            own_of(step),
        )

    def start_pairs(c, carry):
        for step in range(1, planes):

            def hand(i, inner, step=step):
                cols = cols_of(c, i)
                handed[step, :, cols] = weighted(0, step, cols)
                return inner

            lax.fori_loop(0, cut // narrow, hand, 0)
            pair_copy(step, c).start()
        return carry

    await_slabs(0)
    lax.fori_loop(0, cuts, start_pairs, 0)
    for kind in range(CORES):
        start_slab(kind, 0)
    for copy in params + small[1:]:
        copy.start()
    await_slabs(1)

    def send_piece(c, carry):
        for step in range(1, planes):
            pair_copy(step, c).wait_recv()

            def add(i, inner, step=step):
                cols = cols_of(c, i)
                total = weighted(1, step, cols).astype(jnp.float32)
                total = total + taken[step, :, cols].astype(jnp.float32)
                outgoing[step - 1, :, cols] = coded(total)
                return inner

            lax.fori_loop(0, cut // narrow, add, 0)
            grad_copy(step, c).start()
        return carry

    @pl.when(core > 0)
    def _():
        lax.fori_loop(0, cuts, send_piece, 0)

    def pass_up():
        @pl.when(z > 0)
        def _():
            pl.semaphore_wait(chain.at[0], 1)

        @pl.when(z < depth - 1)
        def _():
            signal(chain.at[0], "fs", me + across)

    def pass_down():
        @pl.when(z < depth - 1)
        def _():
            pl.semaphore_wait(chain.at[1], 1)

        @pl.when(z > 0)
        def _():
            signal(chain.at[1], "fs", me - across)

    @pl.when(z < depth // 2)
    def _():
        pass_up()
        pass_down()

    @pl.when(z >= depth // 2)
    def _():
        pass_down()
        pass_up()

    pltpu.make_async_copy(
        grads_hbm.at[0, pl.ds(0, CORES)], grads.at[:, 0], slab_sem.at[CORES]
    ).wait()

    def hand_own(i, carry):
        cols = pl.ds(pl.multiple_of(i * narrow, narrow), narrow)
        handed[0, :, cols] = weighted(0, 0, cols)
        return carry

    lax.fori_loop(0, columns // narrow, hand_own, 0)
    own_copy.start()
    for copy in small[1:]:
        copy.wait()
    own_copy.wait_recv()

    def gather_own(i, carry):
        cols = pl.ds(pl.multiple_of(i * narrow, narrow), narrow)
        mine = weighted(1, 0, cols).astype(jnp.float32)
        gradient[:, cols] = mine + taken[0, :, cols].astype(jnp.float32)
        return carry

    lax.fori_loop(0, columns // narrow, gather_own, 0)
    for copy in params:
        copy.wait()

    span = layer.shape[1]
    lane = lax.broadcasted_iota(jnp.int32, (rows, span), 1)
    term = lane // rows
    inside = lane % rows == lax.broadcasted_iota(jnp.int32, (rows, span), 0)

    def lay(h, carry):
        high = jnp.zeros((rows, span), jnp.float32)
        low = high
        for f in range(5):
            value = jnp.full((rows, span), in_weight[f, h])
            upper = value.astype(jnp.bfloat16).astype(jnp.float32)
            at_high = term == f
            if f < 4:
                at_high = jnp.logical_or(at_high, term == 5 + f)
            high = jnp.where(at_high, upper, high)
            low = jnp.where(term == 9 + f, value - upper, low)
        block = jnp.where(inside, high + low, 0.0)
        layer[pl.ds(pl.multiple_of(h * rows, rows), rows), :] = block.astype(jnp.bfloat16)
        return carry

    lax.fori_loop(0, units, lay, 0)
    starts = []
    slopes = []
    for i in range(2):
        start, slope = out_bias[i], 0.0
        for h in range(units):
            start = start + in_bias[h] * out_weight[i, h]
            slope = slope + in_weight[5, h] * out_weight[i, h]
        starts.append(start)
        slopes.append(slope)

    @pl.when(core == 0)
    def _():
        pl.semaphore_wait(go, 1)
        lax.fori_loop(0, cuts, send_piece, 0)

    def moments(c, carry):
        for step in range(1, planes):
            grad_copy(step, c).wait_recv()

        @pl.when(jnp.logical_and(core > 0, c == max(cuts - GO_EARLY, 0)))
        def _():
            signal(go, "ep", partner)

        def one(i, inner):
            grad_acc, mom_acc = inner
            cols = cols_of(c, i)
            total = gradient[:, cols]
            for step in range(1, planes):
                total = total + decoded(arrived[step - 1, :, cols])
            mom_next = MOMENTUM_DECAY * mom[:, cols] + (1.0 - MOMENTUM_DECAY) * total
            gradient[:, cols] = total
            mom[:, cols] = mom_next
            second[:, cols] = (
                SECOND_DECAY * second[:, cols] + (1.0 - SECOND_DECAY) * total * total
            )
            return grad_acc + folded(total * total), mom_acc + folded(mom_next * mom_next)

        return lax.fori_loop(0, cut // narrow, one, carry)

    zero = jnp.zeros((SUBLANES, LANES), jnp.float32)
    grad_acc, mom_acc = lax.fori_loop(0, cuts, moments, (zero, zero))
    sums[me, 0] = grad_acc
    sums[me, 1] = mom_acc
    for step in range(1, shards):
        remote(
            sums.at[me], sums.at[me], sum_sem.at[0], sum_sem.at[1], "fs", (me + step) % shards
        ).start()
    others = sums.at[pl.ds(0, shards - 1)]
    all_sums = remote(others, others, sum_sem.at[0], sum_sem.at[1], "fs", (me + 1) % shards)
    all_sums.wait_recv()

    entries = rows * columns * shards
    totals = sums[0]
    for s in range(1, shards):
        totals = totals + sums[s]
    mean = jnp.sum(totals, axis=(1, 2), keepdims=True) / entries + NORM_EPS
    inverse = lax.rsqrt(mean)
    inv_grad = inverse[0]
    inv_mom = inverse[1]
    log_mom = 0.5 * jnp.log(mean[1])

    width = columns // chunks
    tile = tile_width(width, MOST_TILE)

    def learned_step(cols):
        grad = gradient[:, cols]
        mom_next = mom[:, cols]
        old = weight[:, cols]
        inv_root = lax.rsqrt(second[:, cols] + ROOT_EPS)
        features = (
            grad * inv_grad,
            mom_next * inv_mom,
            mom_next * inv_root,
            grad * inv_root,
        )
        high = [feature.astype(jnp.bfloat16) for feature in features]
        low = [
            (feature - part.astype(jnp.float32)).astype(jnp.bfloat16)
            for feature, part in zip(features, high)
        ]
        terms = [*high, old, *low, *high, old]
        terms = terms + [jnp.zeros_like(old)] * (TERMS - len(terms))
        hidden = jnp.dot(
            layer[...], jnp.concatenate(terms, axis=0), preferred_element_type=jnp.float32
        )
        direction, magnitude = (
            jnp.broadcast_to(start + slope * log_mom, grad.shape)
            for start, slope in zip(starts, slopes)
        )
        for h in range(units):
            floor = -in_bias[h] - in_weight[5, h] * log_mom
            above = jnp.maximum(hidden[h * rows : (h + 1) * rows], floor)
            direction = direction + above * out_weight[0, h]
            magnitude = magnitude + above * out_weight[1, h]
        update = STEP_SCALE * direction * jnp.exp(EXP_SCALE * magnitude)
        return (old.astype(jnp.float32) - update).astype(jnp.bfloat16)

    def rows_of(source):
        return pl.ds(pl.multiple_of(source * rows, rows), rows)

    ways = (
        (across, z < depth - 1),
        (-across, z > 0),
        (1, x < across - 1),
        (-1, x > 0),
    )
    turned = turned_chunks(depth, across, chunks)
    period = chunks // turned if turned else chunks
    along_z = (z, depth, across, (0, 1))
    along_x = (x, across, 1, (2, 3))
    trees = ((along_x, along_z, turned), (along_z, along_x, chunks - turned))

    def in_tree(tree, k):
        if not turned:
            return k >= 0 if tree else k < 0
        low = (chunks - turned) // 2
        chosen = jnp.logical_and(k >= low, k < low + turned)
        return jnp.logical_not(chosen) if tree else chosen

    def block(source, k):
        return gathered.at[rows_of(source), pl.ds(pl.multiple_of(k * width, width), width)]

    def far_sem(tree, source, k):
        if trees[tree][1][1] == 2:
            k = 0
        elif not tree:
            k = k - (chunks - turned) // 2
        return (turned_recv, straight_recv)[tree].at[source, k]

    def send(tree, source, place, k, which):
        for number in which:
            offset, possible = ways[number]
            near = number in trees[tree][0][3]

            @pl.when(possible)
            def _(number=number, offset=offset, near=near):
                piece = block(source, k)
                remote(
                    piece,
                    piece,
                    row_send.at[tree, number],
                    near_recv.at[place - number % 2, k] if near else far_sem(tree, source, k),
                    "fs",
                    me + offset,
                ).start()

    def await_near(source, place, k):
        piece = block(source, k)
        remote(
            piece, piece, row_send.at[0, 0], near_recv.at[place, k], "fs", source
        ).wait_recv()

    def await_far(tree, source, k):
        piece = block(source, k)
        remote(
            piece, piece, row_send.at[0, 0], far_sem(tree, source, k), "fs", source
        ).wait_recv()

    def live(tree, k):
        inside = jnp.logical_and(k >= 0, k < chunks)
        return jnp.logical_and(inside, in_tree(tree, jnp.maximum(k, 0)))

    def near_lag(tree, d):
        return nth(NEAR_LAGS, d) if tree else TURN_LAG * d

    def relay(t, tree):
        first, second, count = trees[tree]
        if not count:
            return
        at, size, stride, (up, down) = first
        other, length, pitch, (up_other, down_other) = second
        for d in range(size - 1, 0, -1):
            k = t - near_lag(tree, d)

            @pl.when(live(tree, k))
            def _(d=d, k=k):
                @pl.when(at >= d)
                def _():
                    source = me - d * stride
                    await_near(source, at - d, k)
                    send(tree, source, at - d, k, (up,) + second[3])

                @pl.when(at + d < size)
                def _():
                    source = me + d * stride
                    await_near(source, at + d - 1, k)
                    send(tree, source, at + d, k, (down,) + second[3])

        for e in range(length - 2, 0, -1):
            k = t - near_lag(tree, size - 1) - nth(FAR_LAGS, e)

            @pl.when(live(tree, k))
            def _(e=e, k=k):
                for level in range(size):

                    @pl.when(jnp.logical_and(other >= e, other < length - 1))
                    def _(level=level):
                        source = level * stride + (other - e) * pitch
                        await_far(tree, source, k)
                        send(tree, source, level, k, (up_other,))

                    @pl.when(jnp.logical_and(other + e < length, other > 0))
                    def _(level=level):
                        source = level * stride + (other + e) * pitch
                        await_far(tree, source, k)
                        send(tree, source, level, k, (down_other,))

    def turn(t, carry):
        @pl.when(t < chunks)
        def _():
            def one(i, inner):
                cols = pl.ds(pl.multiple_of(t * width + i * tile, tile), tile)
                gathered[rows_of(me), cols] = learned_step(cols)
                return inner

            lax.fori_loop(0, width // tile, one, 0)

        for tree in range(2):

            @pl.when(live(tree, t))
            def _(tree=tree):
                send(tree, me, trees[tree][0][0], t, (0, 1, 2, 3))

        for tree in (1, 0):
            relay(t, tree)
        return carry

    reach = max(
        near_lag(tree, first[1] - 1) + (nth(FAR_LAGS, second[1] - 2) if second[1] > 2 else 0)
        for tree, (first, second, count) in enumerate(trees)
        if count
    )
    lax.fori_loop(0, chunks + reach, turn, 0)

    def finish(k, carry):
        for tree in range(2):
            first, second, count = trees[tree]
            _, size, stride, _ = first
            other, length, pitch, _ = second
            if length == 2:
                continue

            @pl.when(in_tree(tree, k))
            def _(tree=tree, size=size, stride=stride, other=other, length=length, pitch=pitch):
                for level in range(size):
                    for place in range(length):
                        below = jnp.logical_and(place < other, other == length - 1)
                        above = jnp.logical_and(place > other, other == 0)

                        @pl.when(jnp.logical_or(below, above))
                        def _(level=level, place=place):
                            await_far(tree, level * stride + place * pitch, k)

        return carry

    lax.fori_loop(0, chunks, finish, 0)
    for tree in range(2):
        (at, size, stride, moves), (other, length, pitch, far_moves), count = trees[tree]
        if not count:
            continue
        span = pl.ds(0, count * width)
        if length == 2:
            for level in range(size):
                source = level * stride + (1 - other) * pitch
                piece = gathered.at[rows_of(source), span]
                remote(
                    piece, piece, row_send.at[0, 0], far_sem(tree, source, 0), "fs", source
                ).wait_recv()

        def drain(number, position, extent, going_up, each):
            for p in range(extent - 1):
                here = p if going_up else extent - 1 - p

                @pl.when(position == here)
                def _(p=p):
                    piece = gathered.at[pl.ds(0, (p + 1) * each * rows), span]
                    remote(
                        piece,
                        piece,
                        row_send.at[tree, number],
                        sum_sem.at[1],
                        "fs",
                        (me + 1) % shards,
                    ).wait_send()

        for number, going_up in zip(moves, (True, False)):
            drain(number, at, size, going_up, 1)
        for number, going_up in zip(far_moves, (True, False)):
            drain(number, other, length, going_up, size)

    whole = remote(handed, taken, pair_send, own_recv, "ep", partner)
    whole.wait_send()
    remote(outgoing, arrived, grad_send, own_recv, "ep", partner).wait_send()
    all_sums.wait_send()


def flush(gathered, mom, second, gathered_hbm, mom_hbm, second_hbm, sem):
    pairs = ((gathered, gathered_hbm), (mom, mom_hbm), (second, second_hbm))
    for i, (src, dst) in enumerate(pairs):
        height = src.shape[0] // largest_divisor(src.shape[0] // 16, 8)
        for n in range(src.shape[0] // height):
            rows = pl.ds(n * height, height)
            pltpu.make_async_copy(src.at[rows], dst.at[0, rows], sem.at[i]).start()
    for i, (src, dst) in enumerate(pairs):
        pltpu.make_async_copy(src, dst.at[0], sem.at[i]).wait()


def per_device(
    groups, shards, grads, counts, weight, mom, second, in_weight, in_bias, out_weight, out_bias
):
    rows, columns = mom.shape[1], mom.shape[2]
    across = max(d for d in range(1, shards + 1) if shards % d == 0 and d * d <= shards)
    depth = shards // across
    planes = groups // CORES
    chunks = largest_divisor(columns // LANES, MOST_CHUNKS)
    cuts = largest_divisor(columns // LANES, MOST_CUTS)
    turned = turned_chunks(depth, across, chunks)
    hbm = pl.BlockSpec(memory_space=pltpu.HBM)
    vmem = pl.BlockSpec(memory_space=pltpu.VMEM)
    held = (2 * shards + 8) * rows * columns
    gathered, new_mom, new_second = pl.pallas_call(
        functools.partial(kernel, groups, depth, across, chunks),
        out_shape=(
            pltpu.VMEM((rows * shards, columns), jnp.bfloat16),
            pltpu.VMEM((rows, columns), jnp.float32),
            pltpu.VMEM((rows, columns), jnp.float32),
        ),
        in_specs=[hbm] * 9,
        out_specs=(vmem, vmem, vmem),
        scratch_shapes=[
            pltpu.SMEM(counts.shape, jnp.int32),
            pltpu.SMEM(in_weight.shape, jnp.float32),
            pltpu.SMEM(in_bias.shape, jnp.float32),
            pltpu.SMEM(out_weight.shape[::-1], jnp.float32),
            pltpu.SMEM(out_bias.shape, jnp.float32),
            pltpu.VMEM((CORES, planes, rows, columns), jnp.bfloat16),
            pltpu.VMEM((rows, columns), jnp.bfloat16),
            pltpu.VMEM((planes, rows, columns), jnp.bfloat16),
            pltpu.VMEM((planes, rows, columns), jnp.bfloat16),
            pltpu.VMEM((planes - 1, rows, columns), jnp.bfloat16),
            pltpu.VMEM((planes - 1, rows, columns), jnp.bfloat16),
            pltpu.VMEM((rows, columns), jnp.float32),
            pltpu.VMEM((shards, 2, SUBLANES, LANES), jnp.float32),
            pltpu.VMEM((in_bias.shape[0] * rows, TERMS * rows), jnp.bfloat16),
            pltpu.SemaphoreType.DMA((5,)),
            pltpu.SemaphoreType.DMA((CORES + 1,)),
            pltpu.SemaphoreType.DMA((3,)),
            pltpu.SemaphoreType.DMA,
            pltpu.SemaphoreType.DMA((planes - 1, cuts)),
            pltpu.SemaphoreType.DMA,
            pltpu.SemaphoreType.DMA,
            pltpu.SemaphoreType.DMA((planes - 1, cuts)),
            pltpu.SemaphoreType.REGULAR((2,)),
            pltpu.SemaphoreType.REGULAR,
            pltpu.SemaphoreType.DMA((2,)),
            pltpu.SemaphoreType.DMA((2, 4)),
            pltpu.SemaphoreType.DMA((max(depth, across) - 1, chunks)),
            pltpu.SemaphoreType.DMA((shards, 1 if depth == 2 else max(turned, 1))),
            pltpu.SemaphoreType.DMA((shards, 1 if across == 2 else chunks)),
        ],
        compiler_params=pltpu.CompilerParams(
            collective_id=0,
            has_side_effects=True,
            vmem_limit_bytes=VMEM_BYTES - held,
        ),
        name="learned_update",
    )(counts, in_weight, in_bias, out_weight.T, out_bias, grads, weight, mom, second)
    return pl.pallas_call(
        flush,
        out_shape=(
            jax.ShapeDtypeStruct((1, rows * shards, columns), jnp.bfloat16),
            jax.ShapeDtypeStruct(mom.shape, jnp.float32),
            jax.ShapeDtypeStruct(second.shape, jnp.float32),
        ),
        in_specs=[vmem] * 3,
        out_specs=(hbm, hbm, hbm),
        scratch_shapes=[pltpu.SemaphoreType.DMA((3,))],
        compiler_params=pltpu.CompilerParams(
            has_side_effects=True, vmem_limit_bytes=FLUSH_BYTES
        ),
        name="flush",
    )(gathered, new_mom, new_second)


def solution(mesh):
    in_specs = (
        P("ep", None, "fs", None),
        P(),
        P("ep", "fs", None),
        P("ep", "fs", None),
        P("ep", "fs", None),
        P(),
        P(),
        P(),
        P(),
    )
    out_specs = (P("ep", None, None), P("ep", "fs", None), P("ep", "fs", None))
    body = functools.partial(per_device, mesh.shape["ep"], mesh.shape["fs"])
    return jax.shard_map(
        body, mesh=mesh, in_specs=in_specs, out_specs=out_specs, check_vma=False
    )
```

```python
import functools

import jax
import jax.numpy as jnp
from jax import lax
from jax.experimental import pallas as pl
from jax.experimental.pallas import tpu as pltpu
from jax.sharding import PartitionSpec as P

MOMENTUM_DECAY = 0.9
SECOND_DECAY = 0.99
NORM_EPS = 1e-06
ROOT_EPS = 1e-08
STEP_SCALE = 0.2
EXP_SCALE = 0.5
LANES = 128
SUBLANES = 8
CORES = 2
MOST_CHUNKS = 14
MOST_CUTS = 7
CODE_SCALE = 512.0
CODE_LEAST = 2.0**-126
GO_EARLY = 3
NEAR_LAGS = (3, 6, 9)
TURN_LAG = 8
FAR_LAGS = (10, 14)
VMEM_BYTES = 67043328
FLUSH_BYTES = 1 << 20
TERMS = 16
MOST_TILE = 1024


def largest_divisor(number, most):
    return max(d for d in range(1, most + 1) if number % d == 0)


def tile_width(columns, most):
    return LANES * largest_divisor(columns // LANES, most // LANES)


def turned_chunks(depth, across, chunks):
    def load(turned):
        straight = chunks - turned
        on_x = (across - 1) * (depth * straight + (0 if across == 2 else turned))
        on_z = (depth - 1) * (straight + across * turned)
        return max(on_x, on_z)

    return min(range(chunks + 1), key=load)


def nth(lags, d):
    return lags[d - 1] if d <= len(lags) else lags[-1] * d


def remote(src, dst, send_sem, recv_sem, axis, peer):
    return pltpu.make_async_remote_copy(
        src_ref=src,
        dst_ref=dst,
        send_sem=send_sem,
        recv_sem=recv_sem,
        device_id={axis: peer},
        device_id_type=pl.DeviceIdType.MESH,
    )


def coded(value):
    power = value * CODE_SCALE
    for _ in range(3):
        power = power * power
    return jnp.where(value < 0.0, -power, power).astype(jnp.bfloat16)


def decoded(code):
    code = code.astype(jnp.float32)
    fourth = lax.rsqrt(lax.rsqrt(jnp.maximum(jnp.abs(code), CODE_LEAST)))
    size = fourth * lax.rsqrt(fourth) * (1.0 / CODE_SCALE)
    return jnp.where(code == 0.0, 0.0, jnp.where(code < 0.0, -size, size))


def folded(value):
    rows, columns = value.shape
    parts = [
        value[i : i + SUBLANES, j : j + LANES]
        for i in range(0, rows, SUBLANES)
        for j in range(0, columns, LANES)
    ]
    while len(parts) > 1:
        parts = [a + b for a, b in zip(parts[::2], parts[1::2])] + parts[len(parts) & ~1 :]
    return parts[0]


def signal(semaphore, axis, peer):
    pl.semaphore_signal(
        semaphore, inc=1, device_id={axis: peer}, device_id_type=pl.DeviceIdType.MESH
    )


def kernel(
    groups,
    depth,
    across,
    chunks,
    counts_hbm,
    in_weight_hbm,
    in_bias_hbm,
    out_weight_hbm,
    out_bias_hbm,
    grads_hbm,
    weight_hbm,
    mom_hbm,
    second_hbm,
    gathered,
    mom,
    second,
    counts,
    in_weight,
    in_bias,
    out_weight,
    out_bias,
    grads,
    weight,
    handed,
    taken,
    outgoing,
    arrived,
    gradient,
    sums,
    layer,
    extra,
    small_sem,
    slab_sem,
    param_sem,
    pair_send,
    pair_recv,
    own_recv,
    grad_send,
    grad_recv,
    chain,
    go,
    sum_sem,
    row_send,
    near_recv,
    turned_recv,
    straight_recv,
    extra_send,
    extra_recv,
):
    shards = depth * across
    planes = groups // CORES
    rows, columns = mom.shape
    units = in_bias.shape[0]
    me_group = lax.axis_index("ep")
    plane = me_group // CORES
    core = me_group % CORES
    partner = plane * CORES + (CORES - 1 - core)
    me = lax.axis_index("fs")
    z = me // across
    x = me % across

    def own_of(step):
        return (plane + step) % planes * CORES + core

    def other_of(step):
        return (plane + step) % planes * CORES + (CORES - 1 - core)

    barrier = pltpu.get_barrier_semaphore()
    signal(barrier, "ep", partner)
    for step in range(1, planes):
        signal(barrier, "ep", own_of(step))
    for step in range(1, across):
        signal(barrier, "fs", z * across + (x + step) % across)

    @pl.when(z < depth - 1)
    def _():
        signal(barrier, "fs", me + across)

    @pl.when(z > 0)
    def _():
        signal(barrier, "fs", me - across)

    small = [
        pltpu.make_async_copy(src, dst, small_sem.at[i])
        for i, (src, dst) in enumerate(
            (
                (counts_hbm, counts),
                (in_weight_hbm, in_weight),
                (in_bias_hbm, in_bias),
                (out_weight_hbm, out_weight),
                (out_bias_hbm, out_bias),
            )
        )
    ]
    def start_slab(kind, step):
        expert = (other_of, own_of)[kind](step)
        sem = slab_sem.at[kind if step else CORES]
        pltpu.make_async_copy(grads_hbm.at[0, expert], grads.at[kind, step], sem).start()

    def await_slabs(kind):
        pltpu.make_async_copy(
            grads_hbm.at[0, pl.ds(0, planes - 1)],
            grads.at[kind, pl.ds(1, planes - 1)],
            slab_sem.at[kind],
        ).wait()

    small[0].start()
    for kind in range(CORES):
        for step in range(1, planes):
            start_slab(kind, step)
    params = [
        pltpu.make_async_copy(src.at[0], dst, param_sem.at[i])
        for i, (src, dst) in enumerate(
            (
                (mom_hbm, mom),
                (second_hbm, second),
                (weight_hbm, weight),
            )
        )
    ]

    cuts = grad_recv.shape[1]
    cut = columns // cuts
    width = columns // chunks
    turned = turned_chunks(depth, across, chunks)
    low = chunks - turned
    doubled = across == 2 and turned > 0
    first_cut = low * width // cut if doubled else 0
    last_cut = -(-(low + turned) * width // cut) if doubled else 0
    peer = me + 1 - 2 * x
    narrow = tile_width(cut, 1024)

    def cols_of(c, i):
        return pl.ds(pl.multiple_of(c * cut + i * narrow, narrow), narrow)

    def piece_of(c):
        return pl.ds(pl.multiple_of(c * cut, cut), cut)

    small[0].wait()

    def share_of(expert):
        total = counts[0, expert]
        for s in range(1, groups):
            total = total + counts[s, expert]
        mine = jnp.full((1, LANES), counts[me_group, expert].astype(jnp.float32))
        return (mine / jnp.full((1, LANES), total.astype(jnp.float32)))[:, :1]

    shares = [
        [share_of(expert_of(step)) for step in range(planes)] for expert_of in (other_of, own_of)
    ]

    def weighted(kind, step, cols):
        value = shares[kind][step] * grads[kind, step, :, cols].astype(jnp.float32)
        return value.astype(jnp.bfloat16)

    near = 1 + (planes - 1) + (across - 1)
    near = near + (z > 0).astype(jnp.int32) + (z < depth - 1).astype(jnp.int32)
    pl.semaphore_wait(barrier, near)

    def pair_copy(step, c):
        return remote(
            handed.at[step, :, piece_of(c)],
            taken.at[step, :, piece_of(c)],
            pair_send,
            pair_recv.at[step - 1, c],
            "ep",
            partner,
        )

    own_copy = remote(handed.at[0], taken.at[0], pair_send, own_recv, "ep", partner)

    def grad_copy(step, c):
        return remote(
            outgoing.at[step - 1, :, piece_of(c)],
            arrived.at[step - 1, :, piece_of(c)],
            grad_send,
            grad_recv.at[step - 1, c],
            "ep",
            own_of(step),
        )

    def start_pairs(n, carry):
        c = (n + first_cut) % cuts
        for step in range(1, planes):

            def hand(i, inner, step=step):
                cols = cols_of(c, i)
                handed[step, :, cols] = weighted(0, step, cols)
                return inner

            lax.fori_loop(0, cut // narrow, hand, 0)
            pair_copy(step, c).start()
        return carry

    await_slabs(0)
    lax.fori_loop(0, cuts, start_pairs, 0)
    for kind in range(CORES):
        start_slab(kind, 0)
    for copy in params + small[1:]:
        copy.start()
    await_slabs(1)

    def send_piece(n, carry):
        c = (n + first_cut) % cuts
        for step in range(1, planes):
            pair_copy(step, c).wait_recv()

            def add(i, inner, step=step):
                cols = cols_of(c, i)
                total = weighted(1, step, cols).astype(jnp.float32)
                total = total + taken[step, :, cols].astype(jnp.float32)
                outgoing[step - 1, :, cols] = coded(total)
                return inner

            lax.fori_loop(0, cut // narrow, add, 0)
            grad_copy(step, c).start()
        return carry

    @pl.when(core > 0)
    def _():
        lax.fori_loop(0, cuts, send_piece, 0)

    def pass_up():
        @pl.when(z > 0)
        def _():
            pl.semaphore_wait(chain.at[0], 1)

        @pl.when(z < depth - 1)
        def _():
            signal(chain.at[0], "fs", me + across)

    def pass_down():
        @pl.when(z < depth - 1)
        def _():
            pl.semaphore_wait(chain.at[1], 1)

        @pl.when(z > 0)
        def _():
            signal(chain.at[1], "fs", me - across)

    @pl.when(z < depth // 2)
    def _():
        pass_up()
        pass_down()

    @pl.when(z >= depth // 2)
    def _():
        pass_down()
        pass_up()

    pltpu.make_async_copy(
        grads_hbm.at[0, pl.ds(0, CORES)], grads.at[:, 0], slab_sem.at[CORES]
    ).wait()

    def hand_own(i, carry):
        cols = pl.ds(pl.multiple_of(i * narrow, narrow), narrow)
        handed[0, :, cols] = weighted(0, 0, cols)
        return carry

    lax.fori_loop(0, columns // narrow, hand_own, 0)
    own_copy.start()
    for copy in small[1:]:
        copy.wait()
    own_copy.wait_recv()

    def gather_own(i, carry):
        cols = pl.ds(pl.multiple_of(i * narrow, narrow), narrow)
        mine = weighted(1, 0, cols).astype(jnp.float32)
        gradient[:, cols] = mine + taken[0, :, cols].astype(jnp.float32)
        return carry

    lax.fori_loop(0, columns // narrow, gather_own, 0)
    for copy in params:
        copy.wait()

    def extra_copy(i):
        return remote(
            extra.at[0, i], extra.at[1, i], extra_send, extra_recv.at[i // 3], "fs", peer
        )

    reached = extra.shape[3]
    bite = tile_width(reached, 1024)

    def spare(i):
        here = pl.multiple_of(i * bite, bite)
        return pl.ds(here, bite), pl.ds(pl.multiple_of(low * width + here, LANES), bite)

    if doubled:

        def share_state(i, carry):
            near_cols, cols = spare(i)
            extra[0, 0, :, near_cols] = coded(mom[:, cols])
            extra[0, 1, :, near_cols] = coded(second[:, cols])
            extra[0, 2, :, near_cols] = weight[:, cols]
            return carry

        lax.fori_loop(0, reached // bite, share_state, 0)
        for i in range(3):
            extra_copy(i).start()

    span = layer.shape[1]
    lane = lax.broadcasted_iota(jnp.int32, (rows, span), 1)
    term = lane // rows
    inside = lane % rows == lax.broadcasted_iota(jnp.int32, (rows, span), 0)

    def lay(h, carry):
        high = jnp.zeros((rows, span), jnp.float32)
        low = high
        for f in range(5):
            value = jnp.full((rows, span), in_weight[f, h])
            upper = value.astype(jnp.bfloat16).astype(jnp.float32)
            at_high = term == f
            if f < 4:
                at_high = jnp.logical_or(at_high, term == 5 + f)
            high = jnp.where(at_high, upper, high)
            low = jnp.where(term == 9 + f, value - upper, low)
        block = jnp.where(inside, high + low, 0.0)
        layer[pl.ds(pl.multiple_of(h * rows, rows), rows), :] = block.astype(jnp.bfloat16)
        return carry

    lax.fori_loop(0, units, lay, 0)
    starts = []
    slopes = []
    for i in range(2):
        start, slope = out_bias[i], 0.0
        for h in range(units):
            start = start + in_bias[h] * out_weight[i, h]
            slope = slope + in_weight[5, h] * out_weight[i, h]
        starts.append(start)
        slopes.append(slope)

    @pl.when(core == 0)
    def _():
        pl.semaphore_wait(go, 1)
        lax.fori_loop(0, cuts, send_piece, 0)

    def moments(n, carry):
        c = (n + first_cut) % cuts
        for step in range(1, planes):
            grad_copy(step, c).wait_recv()

        @pl.when(jnp.logical_and(core > 0, n == max(cuts - GO_EARLY, 0)))
        def _():
            signal(go, "ep", partner)

        def one(i, inner):
            grad_acc, mom_acc = inner
            cols = cols_of(c, i)
            total = gradient[:, cols]
            for step in range(1, planes):
                total = total + decoded(arrived[step - 1, :, cols])
            mom_next = MOMENTUM_DECAY * mom[:, cols] + (1.0 - MOMENTUM_DECAY) * total
            gradient[:, cols] = total
            mom[:, cols] = mom_next
            second[:, cols] = (
                SECOND_DECAY * second[:, cols] + (1.0 - SECOND_DECAY) * total * total
            )
            return grad_acc + folded(total * total), mom_acc + folded(mom_next * mom_next)

        return lax.fori_loop(0, cut // narrow, one, carry)

    zero = jnp.zeros((SUBLANES, LANES), jnp.float32)
    sofar = lax.fori_loop(0, last_cut - first_cut, moments, (zero, zero))
    if doubled:

        def share_gradient(i, carry):
            near_cols, cols = spare(i)
            extra[0, 3, :, near_cols] = coded(gradient[:, cols])
            return carry

        lax.fori_loop(0, reached // bite, share_gradient, 0)
        extra_copy(3).start()
    grad_acc, mom_acc = lax.fori_loop(last_cut - first_cut, cuts, moments, sofar)
    sums[me, 0] = grad_acc
    sums[me, 1] = mom_acc
    for step in range(1, shards):
        remote(
            sums.at[me], sums.at[me], sum_sem.at[0], sum_sem.at[1], "fs", (me + step) % shards
        ).start()
    others = sums.at[pl.ds(0, shards - 1)]
    all_sums = remote(others, others, sum_sem.at[0], sum_sem.at[1], "fs", (me + 1) % shards)
    all_sums.wait_recv()

    entries = rows * columns * shards
    totals = sums[0]
    for s in range(1, shards):
        totals = totals + sums[s]
    mean = jnp.sum(totals, axis=(1, 2), keepdims=True) / entries + NORM_EPS
    inverse = lax.rsqrt(mean)
    inv_grad = inverse[0]
    inv_mom = inverse[1]
    log_mom = 0.5 * jnp.log(mean[1])

    tile = tile_width(width, MOST_TILE)

    def network(grad, mom_next, second_next, old):
        inv_root = lax.rsqrt(second_next + ROOT_EPS)
        features = (
            grad * inv_grad,
            mom_next * inv_mom,
            mom_next * inv_root,
            grad * inv_root,
        )
        high = [feature.astype(jnp.bfloat16) for feature in features]
        low = [
            (feature - part.astype(jnp.float32)).astype(jnp.bfloat16)
            for feature, part in zip(features, high)
        ]
        terms = [*high, old, *low, *high, old]
        terms = terms + [jnp.zeros_like(old)] * (TERMS - len(terms))
        hidden = jnp.dot(
            layer[...], jnp.concatenate(terms, axis=0), preferred_element_type=jnp.float32
        )
        direction, magnitude = (
            jnp.broadcast_to(start + slope * log_mom, grad.shape)
            for start, slope in zip(starts, slopes)
        )
        for h in range(units):
            floor = -in_bias[h] - in_weight[5, h] * log_mom
            above = jnp.maximum(hidden[h * rows : (h + 1) * rows], floor)
            direction = direction + above * out_weight[0, h]
            magnitude = magnitude + above * out_weight[1, h]
        update = STEP_SCALE * direction * jnp.exp(EXP_SCALE * magnitude)
        return (old.astype(jnp.float32) - update).astype(jnp.bfloat16)

    def learned_step(cols):
        return network(gradient[:, cols], mom[:, cols], second[:, cols], weight[:, cols])

    def doubled_step(slot, cols):
        mom_before, second_before, grad = (
            decoded(extra[slot, i, :, cols]) for i in (0, 1, 3)
        )
        return network(
            grad,
            MOMENTUM_DECAY * mom_before + (1.0 - MOMENTUM_DECAY) * grad,
            SECOND_DECAY * second_before + (1.0 - SECOND_DECAY) * grad * grad,
            extra[slot, 2, :, cols],
        )

    def rows_of(source):
        return pl.ds(pl.multiple_of(source * rows, rows), rows)

    ways = (
        (across, z < depth - 1),
        (-across, z > 0),
        (1, x < across - 1),
        (-1, x > 0),
    )
    along_z = (z, depth, across, (0, 1))
    along_x = (x, across, 1, (2, 3))
    trees = ((along_x, along_z, turned), (along_z, along_x, chunks - turned))

    def in_tree(tree, k):
        if not turned:
            return k >= 0 if tree else k < 0
        low = chunks - turned
        chosen = jnp.logical_and(k >= low, k < low + turned)
        return jnp.logical_not(chosen) if tree else chosen

    def block(source, k):
        return gathered.at[rows_of(source), pl.ds(pl.multiple_of(k * width, width), width)]

    def far_sem(tree, source, k):
        if trees[tree][1][1] == 2:
            k = 0
        elif not tree:
            k = k - (chunks - turned)
        return (turned_recv, straight_recv)[tree].at[source, k]

    def send(tree, source, place, k, which):
        for number in which:
            offset, possible = ways[number]
            near = number in trees[tree][0][3]

            @pl.when(possible)
            def _(number=number, offset=offset, near=near):
                piece = block(source, k)
                remote(
                    piece,
                    piece,
                    row_send.at[tree, number],
                    near_recv.at[place - number % 2, k] if near else far_sem(tree, source, k),
                    "fs",
                    me + offset,
                ).start()

    def await_near(source, place, k):
        piece = block(source, k)
        remote(
            piece, piece, row_send.at[0, 0], near_recv.at[place, k], "fs", source
        ).wait_recv()

    def await_far(tree, source, k):
        piece = block(source, k)
        remote(
            piece, piece, row_send.at[0, 0], far_sem(tree, source, k), "fs", source
        ).wait_recv()

    def live(tree, k):
        inside = jnp.logical_and(k >= 0, k < chunks)
        return jnp.logical_and(inside, in_tree(tree, jnp.maximum(k, 0)))

    def near_lag(tree, d):
        if tree:
            return nth(NEAR_LAGS, d)
        return 0 if doubled else TURN_LAG * d

    def relay(t, tree):
        first, second, count = trees[tree]
        if not count:
            return
        at, size, stride, (up, down) = first
        other, length, pitch, (up_other, down_other) = second
        for d in range(0 if doubled and not tree else size - 1, 0, -1):
            k = t - near_lag(tree, d)

            @pl.when(live(tree, k))
            def _(d=d, k=k):
                @pl.when(at >= d)
                def _():
                    source = me - d * stride
                    await_near(source, at - d, k)
                    send(tree, source, at - d, k, (up,) + second[3])

                @pl.when(at + d < size)
                def _():
                    source = me + d * stride
                    await_near(source, at + d - 1, k)
                    send(tree, source, at + d, k, (down,) + second[3])

        for e in range(length - 2, 0, -1):
            k = t - near_lag(tree, size - 1) - nth(FAR_LAGS, e)

            @pl.when(live(tree, k))
            def _(e=e, k=k):
                for level in range(size):

                    @pl.when(jnp.logical_and(other >= e, other < length - 1))
                    def _(level=level):
                        source = level * stride + (other - e) * pitch
                        await_far(tree, source, k)
                        send(tree, source, level, k, (up_other,))

                    @pl.when(jnp.logical_and(other + e < length, other > 0))
                    def _(level=level):
                        source = level * stride + (other + e) * pitch
                        await_far(tree, source, k)
                        send(tree, source, level, k, (down_other,))

    def turn(t, carry):
        @pl.when(jnp.logical_and(t < chunks, in_tree(1, t)) if doubled else t < chunks)
        def _():
            def one(i, inner):
                cols = pl.ds(pl.multiple_of(t * width + i * tile, tile), tile)
                gathered[rows_of(me), cols] = learned_step(cols)
                return inner

            lax.fori_loop(0, width // tile, one, 0)

            @pl.when(in_tree(1, t))
            def _():
                send(1, me, trees[1][0][0], t, (0, 1, 2, 3))

        @pl.when(live(0, t))
        def _():
            if not doubled:
                send(0, me, trees[0][0][0], t, (0, 1, 2, 3))
                return

            def one(i, inner):
                slot = i // (width // tile)
                here = i % (width // tile) * tile
                cols = pl.ds(pl.multiple_of(t * width + here, tile), tile)
                near_cols = pl.ds(pl.multiple_of((t - low) * width + here, tile), tile)
                source = me + slot * (peer - me)
                gathered[rows_of(source), cols] = doubled_step(slot, near_cols)
                return inner

            lax.fori_loop(0, 2 * (width // tile), one, 0)
            send(0, me, x, t, (0, 1))
            send(0, peer, x, t, (0, 1))

        for tree in (1, 0):
            relay(t, tree)
        return carry

    reach = max(
        near_lag(tree, first[1] - 1) + (nth(FAR_LAGS, second[1] - 2) if second[1] > 2 else 0)
        for tree, (first, second, count) in enumerate(trees)
        if count
    )
    if doubled:
        states = extra.at[1, pl.ds(0, 3)]
        remote(states, states, extra_send, extra_recv.at[0], "fs", peer).wait_recv()
        extra_copy(3).wait_recv()
    lax.fori_loop(0, chunks + reach, turn, 0)

    def finish(k, carry):
        for tree in range(2):
            first, second, count = trees[tree]
            _, size, stride, _ = first
            other, length, pitch, _ = second
            if length == 2:
                continue

            @pl.when(in_tree(tree, k))
            def _(tree=tree, size=size, stride=stride, other=other, length=length, pitch=pitch):
                for level in range(size):
                    for place in range(length):
                        below = jnp.logical_and(place < other, other == length - 1)
                        above = jnp.logical_and(place > other, other == 0)

                        @pl.when(jnp.logical_or(below, above))
                        def _(level=level, place=place):
                            await_far(tree, level * stride + place * pitch, k)

        return carry

    lax.fori_loop(0, chunks, finish, 0)
    for tree in range(2):
        (at, size, stride, moves), (other, length, pitch, far_moves), count = trees[tree]
        if not count:
            continue
        span = pl.ds(0, count * width)
        if length == 2:
            for level in range(size):
                source = level * stride + (1 - other) * pitch
                piece = gathered.at[rows_of(source), span]
                remote(
                    piece, piece, row_send.at[0, 0], far_sem(tree, source, 0), "fs", source
                ).wait_recv()

        def drain(number, position, extent, going_up, each):
            for p in range(extent - 1):
                here = p if going_up else extent - 1 - p

                @pl.when(position == here)
                def _(p=p):
                    piece = gathered.at[pl.ds(0, (p + 1) * each * rows), span]
                    remote(
                        piece,
                        piece,
                        row_send.at[tree, number],
                        sum_sem.at[1],
                        "fs",
                        (me + 1) % shards,
                    ).wait_send()

        for number, going_up in zip(moves, (True, False)):
            if tree or not doubled:
                drain(number, at, size, going_up, 1)
        for number, going_up in zip(far_moves, (True, False)):
            drain(number, other, length, going_up, size)

    if doubled:
        remote(extra.at[0], extra.at[1], extra_send, extra_recv.at[0], "fs", peer).wait_send()
    whole = remote(handed, taken, pair_send, own_recv, "ep", partner)
    whole.wait_send()
    remote(outgoing, arrived, grad_send, own_recv, "ep", partner).wait_send()
    all_sums.wait_send()


def flush(gathered, mom, second, gathered_hbm, mom_hbm, second_hbm, sem):
    pairs = ((gathered, gathered_hbm), (mom, mom_hbm), (second, second_hbm))
    for i, (src, dst) in enumerate(pairs):
        height = src.shape[0] // largest_divisor(src.shape[0] // 16, 8)
        for n in range(src.shape[0] // height):
            rows = pl.ds(n * height, height)
            pltpu.make_async_copy(src.at[rows], dst.at[0, rows], sem.at[i]).start()
    for i, (src, dst) in enumerate(pairs):
        pltpu.make_async_copy(src, dst.at[0], sem.at[i]).wait()


def per_device(
    groups, shards, grads, counts, weight, mom, second, in_weight, in_bias, out_weight, out_bias
):
    rows, columns = mom.shape[1], mom.shape[2]
    across = max(d for d in range(1, shards + 1) if shards % d == 0 and d * d <= shards)
    depth = shards // across
    planes = groups // CORES
    chunks = largest_divisor(columns // LANES, MOST_CHUNKS)
    cuts = largest_divisor(columns // LANES, MOST_CUTS)
    turned = turned_chunks(depth, across, chunks)
    hbm = pl.BlockSpec(memory_space=pltpu.HBM)
    vmem = pl.BlockSpec(memory_space=pltpu.VMEM)
    held = (2 * shards + 8) * rows * columns
    gathered, new_mom, new_second = pl.pallas_call(
        functools.partial(kernel, groups, depth, across, chunks),
        out_shape=(
            pltpu.VMEM((rows * shards, columns), jnp.bfloat16),
            pltpu.VMEM((rows, columns), jnp.float32),
            pltpu.VMEM((rows, columns), jnp.float32),
        ),
        in_specs=[hbm] * 9,
        out_specs=(vmem, vmem, vmem),
        scratch_shapes=[
            pltpu.SMEM(counts.shape, jnp.int32),
            pltpu.SMEM(in_weight.shape, jnp.float32),
            pltpu.SMEM(in_bias.shape, jnp.float32),
            pltpu.SMEM(out_weight.shape[::-1], jnp.float32),
            pltpu.SMEM(out_bias.shape, jnp.float32),
            pltpu.VMEM((CORES, planes, rows, columns), jnp.bfloat16),
            pltpu.VMEM((rows, columns), jnp.bfloat16),
            pltpu.VMEM((planes, rows, columns), jnp.bfloat16),
            pltpu.VMEM((planes, rows, columns), jnp.bfloat16),
            pltpu.VMEM((planes - 1, rows, columns), jnp.bfloat16),
            pltpu.VMEM((planes - 1, rows, columns), jnp.bfloat16),
            pltpu.VMEM((rows, columns), jnp.float32),
            pltpu.VMEM((shards, 2, SUBLANES, LANES), jnp.float32),
            pltpu.VMEM((in_bias.shape[0] * rows, TERMS * rows), jnp.bfloat16),
            pltpu.VMEM((2, 4, rows, max(turned, 1) * (columns // chunks)), jnp.bfloat16),
            pltpu.SemaphoreType.DMA((5,)),
            pltpu.SemaphoreType.DMA((CORES + 1,)),
            pltpu.SemaphoreType.DMA((3,)),
            pltpu.SemaphoreType.DMA,
            pltpu.SemaphoreType.DMA((planes - 1, cuts)),
            pltpu.SemaphoreType.DMA,
            pltpu.SemaphoreType.DMA,
            pltpu.SemaphoreType.DMA((planes - 1, cuts)),
            pltpu.SemaphoreType.REGULAR((2,)),
            pltpu.SemaphoreType.REGULAR,
            pltpu.SemaphoreType.DMA((2,)),
            pltpu.SemaphoreType.DMA((2, 4)),
            pltpu.SemaphoreType.DMA((max(depth, across) - 1, chunks)),
            pltpu.SemaphoreType.DMA((shards, 1 if depth == 2 else max(turned, 1))),
            pltpu.SemaphoreType.DMA((shards, 1 if across == 2 else chunks)),
            pltpu.SemaphoreType.DMA,
            pltpu.SemaphoreType.DMA((2,)),
        ],
        compiler_params=pltpu.CompilerParams(
            collective_id=0,
            has_side_effects=True,
            vmem_limit_bytes=VMEM_BYTES - held,
        ),
        name="learned_update",
    )(counts, in_weight, in_bias, out_weight.T, out_bias, grads, weight, mom, second)
    return pl.pallas_call(
        flush,
        out_shape=(
            jax.ShapeDtypeStruct((1, rows * shards, columns), jnp.bfloat16),
            jax.ShapeDtypeStruct(mom.shape, jnp.float32),
            jax.ShapeDtypeStruct(second.shape, jnp.float32),
        ),
        in_specs=[vmem] * 3,
        out_specs=(hbm, hbm, hbm),
        scratch_shapes=[pltpu.SemaphoreType.DMA((3,))],
        compiler_params=pltpu.CompilerParams(
            has_side_effects=True, vmem_limit_bytes=FLUSH_BYTES
        ),
        name="flush",
    )(gathered, new_mom, new_second)


def solution(mesh):
    in_specs = (
        P("ep", None, "fs", None),
        P(),
        P("ep", "fs", None),
        P("ep", "fs", None),
        P("ep", "fs", None),
        P(),
        P(),
        P(),
        P(),
    )
    out_specs = (P("ep", None, None), P("ep", "fs", None), P("ep", "fs", None))
    body = functools.partial(per_device, mesh.shape["ep"], mesh.shape["fs"])
    return jax.shard_map(
        body, mesh=mesh, in_specs=in_specs, out_specs=out_specs, check_vma=False
    )
```
